32 devices in a mesh: stream: 32 (over z, y, x, core), item: 1.
Axes of the slice: x: 2, y: 2, z: 4, core: 2. Of those that a mesh axis runs over, the one named last changes fastest.
Arguments:
- event_items: int32 [131072], P('stream'), may hold values from 0 to 262143, as said below
- event_sessions: int32 [131072], P('stream'), may hold values from 0 to 8191, never falling along the last dimension, each value on 1 to 64 neighbouring positions
- sketch_bits: int32 [15, 262144], P(None, 'item'), may hold values from 0 to 262143
Outputs:
- sketch: float32 [128, 256], P('stream')
The draws below stay inside these ranges and needn't reach their ends.
Inputs may be any that keep to these rules, and one draw needn't show every extreme that they name: `event_items`: item 262144 - 1 occurs at least once.
All inputs are finite; a program needn't handle non-finite values.
Results may differ from the reference program's by a relative error of at most 0.0006.
Values may be sent and summed in bfloat16 or wider, within the bound.
A program may use at most 128 MiB of HBM per device.

```python
import math
import jax
import jax.numpy as jnp
import numpy as np
from jax import lax

ITEMS = 262144
SKETCH = 256
WINDOW = 15
WORDS = 15
EVENTS = 131072
ROWS = 128


def draw_event_items(key, part):
    first_key, second_key, third_key = jax.random.split(jax.random.fold_in(key, 7), 3)
    picker = jax.random.randint(first_key, (EVENTS,), 0, 2)
    row_items = jax.random.randint(second_key, (EVENTS,), 0, ROWS)
    wide_items = jax.random.randint(third_key, (EVENTS,), 0, ITEMS)
    chosen = jnp.where(picker == 0, row_items, wide_items)
    return chosen.at[EVENTS // 2].set(ITEMS - 1).astype(jnp.int32)


def place_ends(values, own_key, low, high):
    dims = values.shape
    index_at = [jax.random.randint(jax.random.fold_in(own_key, axis), (), 0, dims[axis]) for axis in range(len(dims))]
    values = values.at[tuple(index_at)].set(low)
    longest = dims.index(max(dims))
    index_at[longest] = (index_at[longest] + 1) % dims[longest]
    return values.at[tuple(index_at)].set(high)


def split_up(count, total, most, slope):
    weights = [(1 << 20) // math.isqrt(rank ** slope) + 1 for rank in range(2, count + 1)]
    rest, given = total - most - (count - 1), [1] * (count - 1)
    while rest > 0:
        candidates = [i for i in range(count - 1) if given[i] < most]
        pool, remaining = sum([weights[i] for i in candidates]), rest
        for i in candidates:
            more = min(most - given[i], max(1, remaining * weights[i] // pool), rest)
            given[i] = given[i] + more
            rest = rest - more
    return np.array([most] + given)


def uneven(rng, count, total, bound, lean):
    if count == 2:
        one = jax.random.randint(rng, (), max(1, total - bound), min(bound, total - 1) + 1)
        return jnp.stack([one, total - one])
    tallies = jnp.asarray(split_up(count, total, bound, lean), jnp.int32)
    pairs = (count - 1) // 2
    giver, receiver = tallies[1:1 + 2 * pairs:2], tallies[2:2 + 2 * pairs:2]
    room = jnp.minimum(giver - 1, bound - receiver)
    passed = jax.random.randint(jax.random.fold_in(rng, 1), (pairs,), 0, 1 << 20) % (room + 1)
    tallies = tallies.at[1:1 + 2 * pairs:2].set(giver - passed).at[2:2 + 2 * pairs:2].set(receiver + passed)
    return tallies[jax.random.permutation(jax.random.fold_in(rng, 2), count)]


def setup_inputs(seed: int = 0) -> dict:
    key_of = jax.random.split(jax.random.key(seed), 4)
    return {
        "event_items": draw_event_items(jax.random.fold_in(key_of[3], 71), 0),
        "event_sessions": jnp.searchsorted(jnp.cumsum(uneven(key_of[1], EVENTS // 16, EVENTS, 64, 0)), jnp.arange(EVENTS), side="right").astype(jnp.int32),
        "sketch_bits": place_ends(jax.random.randint(key_of[2], (WORDS, ITEMS), 0, 2 ** 18), jax.random.fold_in(key_of[2], 1), 0, (2 ** 18) - 1).astype(jnp.int32),
    }


def pointwise(count_block, row_margin, col_margin, pair_total):
    log_ratio = jnp.log(jnp.maximum(count_block, 1.0)) + jnp.log(pair_total) - jnp.log(jnp.maximum(row_margin, 1.0)) - jnp.log(jnp.maximum(col_margin, 1.0))
    return jnp.where(count_block > 0, jnp.maximum(log_ratio, 0.0), 0.0)

def sign_table(bit_block, sketch_width):
    word_count = bit_block.shape[0]
    spread = jnp.repeat(bit_block, 18, axis=0, total_repeat_length=word_count * 18)[:sketch_width]
    bit_shift = (jnp.arange(sketch_width, dtype=jnp.int32) % 18)[:, None]
    return (2 * jnp.bitwise_and(jnp.right_shift(spread, bit_shift), 1) - 1).astype(jnp.float32)

def reference(event_items, event_sessions, sketch_bits):
    position = jnp.arange(EVENTS, dtype=jnp.int32)
    partners = []
    weights = []
    for offset in range(1, WINDOW + 1):
        for direction in (1, -1):
            other_pos = position + direction * offset
            inside = (other_pos >= 0) & (other_pos < EVENTS)
            clipped = jnp.clip(other_pos, 0, EVENTS - 1).astype(jnp.int32)
            linked = inside & (event_sessions[clipped] == event_sessions)
            partners.append(event_items[clipped])
            weights.append(linked.astype(jnp.float32))
    partner_all = jnp.concatenate(partners)
    weight_all = jnp.concatenate(weights)
    owner_all = jnp.tile(event_items, 2 * WINDOW)
    margin = jnp.zeros((ITEMS,), jnp.float32).at[partner_all].add(weight_all)
    hit_row = owner_all < ROWS
    counts = jnp.zeros((ROWS, ITEMS), jnp.float32).at[jnp.where(hit_row, owner_all, 0), partner_all].add(jnp.where(hit_row, weight_all, 0.0))
    pair_total = jnp.sum(margin)
    row_margin = margin[:ROWS]
    block_width = math.gcd(ITEMS, 8192)

    def accumulate(block_index, summed):
        first_col = (block_index * block_width).astype(jnp.int32)
        count_block = lax.dynamic_slice_in_dim(counts, first_col, block_width, 1)
        col_margin = lax.dynamic_slice_in_dim(margin, first_col, block_width, 0)
        bit_block = lax.dynamic_slice_in_dim(sketch_bits, first_col, block_width, 1)
        positive = pointwise(count_block, row_margin[:, None], col_margin[None, :], pair_total)
        sign_rows = sign_table(bit_block, SKETCH)
        return summed + lax.dot_general(positive, sign_rows, (((1,), (1,)), ((), ())), precision=lax.Precision.HIGHEST, preferred_element_type=jnp.float32)
    summed = lax.fori_loop(0, ITEMS // block_width, accumulate, jnp.zeros((ROWS, SKETCH), jnp.float32))
    return summed / math.sqrt(EVENTS)
```

```python
import functools
import math

import jax
import jax.numpy as jnp
from jax import lax
from jax.experimental import pallas as pl
from jax.experimental.pallas import tpu as pltpu
from jax.sharding import PartitionSpec as P

WINDOW = 15
ITEM_BITS = 18
LANES = 128
BITS_PER_WORD = 18
BIG = 1.0e6
NT = (((1,), (1,)), ((), ()))
VMEM = pl.BlockSpec(memory_space=pltpu.VMEM)


def one_where(mask):
    return jnp.where(mask, 1.0, 0.0).astype(jnp.bfloat16)


def head_kernel(rows, blocks, code_ref, out_ref):
    ext = rows + 8
    out_ref[...] = jnp.zeros_like(out_ref)
    sub = lax.broadcasted_iota(jnp.int32, (LANES, LANES), 0)
    lane = lax.broadcasted_iota(jnp.int32, (LANES, LANES), 1)
    item_mask = (1 << ITEM_BITS) - 1
    ids = lax.broadcasted_iota(jnp.int32, (ext, LANES), 0)

    def hot(code):
        item = jnp.where(code < 0, rows + 1, code & item_mask)
        item = jnp.where(item >= rows, rows + 1, item)
        return one_where((ids == item) | (ids == rows))

    def step(b, unused):
        own = code_ref[pl.ds(b + 1, 1), :]
        own_session = own >> ITEM_BITS
        links = jnp.zeros((ext, LANES), jnp.float32)
        for o in (-1, 0, 1):
            other = code_ref[pl.ds(b + 1 + o, 1), :]
            other_session = jnp.broadcast_to(other >> ITEM_BITS, (LANES, LANES)).T
            gap = o * LANES + sub - lane
            linked = (other_session == own_session) & (jnp.abs(gap) <= WINDOW) & (gap != 0)
            links += jnp.dot(hot(other), one_where(linked), preferred_element_type=jnp.float32)
        out_ref[...] += lax.dot_general(
            links.astype(jnp.bfloat16), hot(own), NT, preferred_element_type=jnp.float32
        )
        return unused

    lax.fori_loop(0, blocks, step, 0)


def take_windows(code_ref, length, start):
    whole, part = start >> 3, start & 7
    bits = max(1, (length // 8 - 1).bit_length())
    keep = 8 * ((1 << (bits - 1)) + 4)
    value = None
    for bit in reversed(range(bits)):
        step = 8 << bit
        keep = 8 * ((1 << bit) + 4)
        chosen = ((whole >> bit) & 1) == 1
        if value is None:
            low, high = code_ref[0:keep, :], code_ref[step : step + keep, :]
        else:
            low, high = value[0:keep], value[step : step + keep]
        value = jnp.where(chosen, high, low)
    for bit in (2, 1, 0):
        chosen = ((part >> bit) & 1) == 1
        value = jnp.where(chosen, pltpu.roll(value, value.shape[0] - (1 << bit), 0), value)
    return value[0:32]


def tile_kernel(rows, length, half, base_ref, code_ref, count_ref, margin_ref, key_ref):
    item_mask = (1 << ITEM_BITS) - 1
    base = base_ref[0]
    count_ref[...] = jnp.zeros_like(count_ref)
    margin_ref[...] = jnp.zeros_like(margin_ref)
    band = 2 * half
    band_rows = band // LANES
    chunk = 8 * math.gcd(length // 8, 16)

    def fill(c, tops):
        at = pl.multiple_of(c * chunk, chunk)
        item = code_ref[pl.ds(at + 16, chunk), :] & item_mask
        place = (at + lax.broadcasted_iota(jnp.int32, (chunk, LANES), 0)).astype(jnp.float32)
        new = []
        for s in range(2):
            local = item - base - s * band
            mine = (local >= 0) & (local < band) & (item >= rows)
            key_ref[s, pl.ds(at, chunk), :] = jnp.where(mine, place, BIG)
            new.append(tops[s] + jnp.sum(mine.astype(jnp.int32), axis=0, keepdims=True))
        return tuple(new)

    none = jnp.zeros((1, LANES), jnp.int32)
    tally = lax.fori_loop(0, length // chunk, fill, (none, none))
    trips = (jnp.max(jnp.maximum(tally[0], tally[1])) + 1) // 2

    row_ids = lax.broadcasted_iota(jnp.int32, (rows, 2 * LANES), 0).astype(jnp.float32)
    d_ids = lax.broadcasted_iota(jnp.int32, (32, LANES), 0)
    near = (d_ids >= 1) & (d_ids != 16)
    m_ids = lax.broadcasted_iota(jnp.int32, (max(8, band_rows), 2 * LANES), 0)
    l_ids = lax.broadcasted_iota(jnp.int32, (LANES, 2 * LANES), 0)
    tile = min(half, 512)
    t_ids = lax.broadcasted_iota(jnp.int32, (tile, 2 * LANES), 0)

    def body(unused, state):
        out = []
        for s in range(2):
            first, last = state[2 * s], state[2 * s + 1]
            key = key_ref[s]
            next_first = jnp.min(jnp.where(key > first, key, BIG), axis=0, keepdims=True)
            next_last = jnp.max(jnp.where(key < last, key, -1.0), axis=0, keepdims=True)
            first_ok = next_first < last
            last_ok = next_last > next_first
            out += [next_first, next_last]
            heads, weights, locals_ = [], [], []
            for at, ok in ((next_first, first_ok), (next_last, last_ok)):
                start = jnp.where(ok, at, 0.0).astype(jnp.int32)
                window = take_windows(code_ref, length, start)
                item, session = window & item_mask, window >> ITEM_BITS
                linked = (session == session[16:17]) & near & ok
                heads.append(jnp.where(linked & (item < rows), item, -1).astype(jnp.float32))
                weights.append(jnp.sum(jnp.where(linked, 1.0, 0.0), axis=0, keepdims=True))
                locals_.append(item[16:17] - base - s * band)
            head = jnp.concatenate(heads, axis=1)
            weight = jnp.concatenate(weights, axis=1)
            local = jnp.concatenate(locals_, axis=1)
            links = jnp.zeros((rows, 2 * LANES), jnp.float32)
            for d in range(1, 32):
                if d != 16:
                    links += jnp.where(row_ids == head[d : d + 1], 1.0, 0.0)
            upper = local >= half
            pair = jnp.concatenate(
                [jnp.where(upper, 0.0, links), jnp.where(upper, links, 0.0)], axis=0
            ).astype(jnp.bfloat16)
            inner = jnp.where(upper, local - half, local)
            for t in range(half // tile):
                hot = one_where(t_ids + t * tile == inner)
                count_ref[s, :, t * tile : (t + 1) * tile] += lax.dot_general(
                    pair, hot, NT, preferred_element_type=jnp.float32
                )
            coarse = jnp.where(m_ids == (local >> 7), weight, 0.0).astype(jnp.bfloat16)
            fine = one_where(l_ids == (local & (LANES - 1)))
            margin_ref[s] += lax.dot_general(coarse, fine, NT, preferred_element_type=jnp.float32)
        return tuple(out)

    low = jnp.full((1, LANES), -1.0, jnp.float32)
    high = jnp.full((1, LANES), BIG, jnp.float32)
    lax.fori_loop(0, trips, body, (low, high, low, high))


def sketch_kernel(rows, half, width, scale, flag_ref, count_ref, margin_ref, head_ref, bits_ref, out_ref, log_ref):
    flag = flag_ref[0]
    band_rows = 2 * half // LANES
    row_margin = head_ref[rows : rows + 1, 0:rows]
    first_row = lax.broadcasted_iota(jnp.int32, margin_ref.shape[1:], 0) == 0
    log_ref[0] = jnp.log(jnp.maximum(margin_ref[0] + jnp.where(first_row, row_margin * flag, 0.0), 1.0))
    log_ref[1] = jnp.log(jnp.maximum(margin_ref[1], 1.0))
    row_term = jnp.log(head_ref[rows : rows + 1, rows : rows + 1]) - jnp.log(
        jnp.maximum(head_ref[0:rows, rows : rows + 1], 1.0)
    )
    tile = min(half, 512)
    out_ref[...] = jnp.zeros_like(out_ref)
    shift = lax.broadcasted_iota(jnp.int32, (8, tile), 0)
    head_block = head_ref[0:rows, 0:rows] * flag
    groups = []
    for g in range(width // 8):
        word = 8 * g // BITS_PER_WORD
        split = (word + 1) * BITS_PER_WORD - 8 * g
        groups.append((word, split, 8 * g - word * BITS_PER_WORD))

    def block(s, h, t):
        at = pl.multiple_of(t * tile, tile)
        counts = count_ref[s, h * rows : (h + 1) * rows, pl.ds(at, tile)]
        if s == 0 and h == 0:
            on = jnp.where(t == 0, 1.0, 0.0)
            extra = head_block * on
            if tile > rows:
                extra = jnp.concatenate([extra, jnp.zeros((rows, tile - rows), jnp.float32)], axis=1)
            counts = counts + extra
        first_log = h * (half // LANES) + t * (tile // LANES)
        col_log = jnp.concatenate(
            [log_ref[s, pl.ds(first_log + n, 1), :] for n in range(tile // LANES)], axis=1
        )
        ratio = jnp.log(jnp.maximum(counts, 1.0)) + row_term - col_log
        positive = jnp.where(counts > 0, jnp.maximum(ratio, 0.0), 0.0)
        upper = positive.astype(jnp.bfloat16)
        lower = (positive - upper.astype(jnp.float32)).astype(jnp.bfloat16)
        bit_at = pl.multiple_of(s * 2 * half + h * half + t * tile, tile)
        words = bits_ref[:, pl.ds(bit_at, tile)]
        parts = []
        for word, split, offset in groups:
            now = jnp.broadcast_to(words[word : word + 1], (8, tile))
            where_bit = shift + offset
            if split < 8:
                after = jnp.broadcast_to(words[word + 1 : word + 2], (8, tile))
                now = jnp.where(shift >= split, after, now)
                where_bit = jnp.where(shift >= split, shift - split, where_bit)
            parts.append(jnp.where(((now >> where_bit) & 1) == 1, 1.0, -1.0))
        signs = jnp.concatenate(parts, axis=0).astype(jnp.bfloat16)
        both = jnp.concatenate([upper, lower], axis=0)
        product = lax.dot_general(both, signs, NT, preferred_element_type=jnp.float32)
        out_ref[...] += product[0:rows] + product[rows:]

    for s in range(2):
        for h in range(2):

            def step(t, unused, s=s, h=h):
                block(s, h, t)
                return unused

            lax.fori_loop(0, half // tile, step, 0)
    out_ref[...] = out_ref[...] * scale


def local(event_items, event_sessions, sketch_bits):
    slabs = lax.axis_size("stream")
    slab = event_items.shape[0]
    total_events = slab * slabs
    words, band_size = sketch_bits.shape
    owned = band_size // slabs
    rows, width, half = 128, 256, owned // 4
    me = lax.axis_index("stream")
    own_start = me * owned
    first_id = lax.axis_index("item") * band_size + own_start
    blocks = slab // LANES
    length = total_events // LANES

    events = lax.all_gather(jnp.stack([event_items, event_sessions])[None], "stream", axis=0, tiled=True)
    code = events[:, 0] | (events[:, 1] << ITEM_BITS)
    flat = code.reshape(length, LANES)
    padded = jnp.pad(flat, ((1, 1), (0, 0)), constant_values=-1)
    own = lax.dynamic_slice_in_dim(padded, me * blocks, blocks + 2, 0)
    head = pl.pallas_call(
        functools.partial(head_kernel, rows, blocks),
        out_shape=jax.ShapeDtypeStruct((rows + 8, rows + 8), jnp.float32),
        in_specs=[VMEM],
        out_specs=VMEM,
        name="head_counts",
    )(own)
    head = lax.psum(head, "stream")

    deep = code.reshape(LANES, length).T
    before = jnp.pad(deep[length - 16 :, :-1], ((0, 0), (1, 0)), constant_values=-1)
    after = jnp.pad(deep[:16, 1:], ((0, 0), (0, 1)), constant_values=-1)
    deep = jnp.concatenate([before, deep, after], axis=0)
    band_rows = max(8, 2 * half // LANES)
    counts, margins = pl.pallas_call(
        functools.partial(tile_kernel, rows, length, half),
        out_shape=(
            jax.ShapeDtypeStruct((2, 2 * rows, half), jnp.float32),
            jax.ShapeDtypeStruct((2, band_rows, LANES), jnp.float32),
        ),
        in_specs=[pl.BlockSpec(memory_space=pltpu.SMEM), VMEM],
        out_specs=(VMEM, VMEM),
        scratch_shapes=[pltpu.VMEM((2, length, LANES), jnp.float32)],
        cost_estimate=pl.CostEstimate(flops=40_000_000_000, bytes_accessed=5_000_000, transcendentals=0),
        name="tile_counts",
    )(first_id.astype(jnp.int32)[None], deep)

    own_bits = lax.dynamic_slice_in_dim(sketch_bits, own_start, owned, 1)
    own_bits = jnp.pad(own_bits, ((0, 16 - words), (0, 0)))
    flag = jnp.where(first_id == 0, 1.0, 0.0).astype(jnp.float32)[None]
    partial_sketch = pl.pallas_call(
        functools.partial(sketch_kernel, rows, half, width, 1.0 / math.sqrt(total_events)),
        out_shape=jax.ShapeDtypeStruct((rows, width), jnp.float32),
        in_specs=[pl.BlockSpec(memory_space=pltpu.SMEM)] + [VMEM] * 4,
        out_specs=VMEM,
        scratch_shapes=[pltpu.VMEM((2, band_rows, LANES), jnp.float32)],
        name="sketch_tile",
    )(flag, counts, margins, head, own_bits)
    own_rows = lax.psum_scatter(partial_sketch, "stream", scatter_dimension=0, tiled=True)
    if lax.axis_size("item") > 1:
        own_rows = lax.psum(own_rows, "item")
    return own_rows


def solution(mesh):
    placed = (P("stream"), P("stream"), P(None, "item"))
    return jax.shard_map(
        local, mesh=mesh, in_specs=placed, out_specs=P("stream", None), check_vma=False
    )
```

```python
import functools
import math

import jax
import jax.numpy as jnp
from jax import lax
from jax.experimental import pallas as pl
from jax.experimental.pallas import tpu as pltpu
from jax.sharding import PartitionSpec as P

WINDOW = 15
ITEM_BITS = 18
LANES = 128
BITS_PER_WORD = 18
BIG = 1.0e6
NT = (((1,), (1,)), ((), ()))
VMEM = pl.BlockSpec(memory_space=pltpu.VMEM)


def one_where(mask):
    return jnp.where(mask, 1.0, 0.0).astype(jnp.bfloat16)


def greet_all(slabs, me):
    barrier = pltpu.get_barrier_semaphore()

    def signal(k, unused):
        pl.semaphore_signal(
            barrier, inc=1, device_id={"stream": lax.rem(me + k, slabs)}, device_id_type=pl.DeviceIdType.MESH
        )
        return unused

    lax.fori_loop(1, slabs, signal, 0)
    return barrier


def send(src, dst, send_sem, recv_sem, to):
    return pltpu.make_async_remote_copy(
        src_ref=src,
        dst_ref=dst,
        send_sem=send_sem,
        recv_sem=recv_sem,
        device_id={"stream": to},
        device_id_type=pl.DeviceIdType.MESH,
    )


def each(low, high, do):
    def step(k, unused):
        do(k)
        return unused

    lax.fori_loop(low, high, step, 0)


def exchange(slabs, me, out_ref, in_ref, send_sems, recv_sems, start):
    def copy(k):
        to = lax.rem(me + k, slabs)
        return send(out_ref.at[to], in_ref.at[me], send_sems.at[k], recv_sems.at[k], to)

    if start:
        each(1, slabs, lambda k: copy(k).start())
        in_ref[me] = out_ref[me]
    else:
        each(1, slabs, lambda k: copy(k).wait())


def gather_kernel(
    slabs, rows, blocks, own_ref, all_ref, head_ref, halo_ref, item_ref, session_ref, links_ref, total_ref,
    head_out, head_in, far_send, far_recv, near_send, near_recv, halo_send, halo_recv, head_send, head_recv,
):
    me = lax.axis_index("stream")
    partner = me + 1 - 2 * lax.rem(me, 2)
    after, before = lax.rem(me + 1, slabs), lax.rem(me + slabs - 1, slabs)
    barrier = greet_all(slabs, me)
    pl.semaphore_wait(barrier, slabs - 1)

    low_halo = send(own_ref.at[:, blocks - 8 : blocks], halo_ref.at[0], halo_send.at[0], halo_recv.at[0], after)
    high_halo = send(own_ref.at[:, 0:8], halo_ref.at[1], halo_send.at[1], halo_recv.at[1], before)
    low_halo.start()
    high_halo.start()

    def far(k):
        return send(own_ref, all_ref.at[me], far_send.at[k], far_recv.at[k], lax.rem(me + 2 * k, slabs))

    def near(k):
        source = lax.rem(me + 2 * slabs - 2 * k, slabs)
        return send(all_ref.at[source], all_ref.at[source], near_send.at[k], near_recv.at[k], partner)

    own_near = send(own_ref, all_ref.at[me], near_send.at[0], near_recv.at[0], partner)
    own_near.start()
    each(1, slabs // 2, lambda k: far(k).start())
    all_ref[me] = own_ref[...]

    item_ref[8 : 8 + blocks] = own_ref[0]
    session_ref[8 : 8 + blocks] = own_ref[1]
    low_halo.wait()
    high_halo.wait()
    item_ref[0:8] = halo_ref[0, 0]
    item_ref[8 + blocks : 16 + blocks] = halo_ref[1, 0]
    session_ref[0:8] = jnp.where(me == 0, -1, halo_ref[0, 1])
    session_ref[8 + blocks : 16 + blocks] = jnp.where(me == slabs - 1, -1, halo_ref[1, 1])

    sub = lax.broadcasted_iota(jnp.int32, (LANES, LANES), 0)
    lane = lax.broadcasted_iota(jnp.int32, (LANES, LANES), 1)
    low_lane = lax.broadcasted_iota(jnp.int32, (1, LANES), 1) < LANES // 2
    ids = lax.broadcasted_iota(jnp.int32, (rows, LANES), 0)
    gaps = (sub - LANES // 2 - lane, sub + LANES // 2 - lane)
    in_reach = [(jnp.abs(gap) <= WINDOW) & (gap != 0) for gap in gaps]
    ones = jnp.ones((8, 2 * LANES), jnp.float32).astype(jnp.bfloat16)
    links_ref[...] = jnp.zeros_like(links_ref)
    total_ref[...] = jnp.zeros_like(total_ref)

    def block(b, unused):
        def around(ref):
            turned = [pltpu.roll(ref[pl.ds(b + o, 1)], LANES // 2, 1) for o in (7, 8, 9)]
            return (
                jnp.where(low_lane, turned[0], turned[1]),
                jnp.where(low_lane, turned[1], turned[2]),
            )

        own_item, own_session = item_ref[pl.ds(b + 8, 1)], session_ref[pl.ds(b + 8, 1)]
        hot = jnp.concatenate([one_where(ids == item) for item in around(item_ref)], axis=1)
        linked = jnp.concatenate(
            [
                one_where((jnp.broadcast_to(session, (LANES, LANES)).T == own_session) & reach)
                for session, reach in zip(around(session_ref), in_reach)
            ],
            axis=0,
        )
        links = jnp.dot(jnp.concatenate([hot, ones], axis=0), linked, preferred_element_type=jnp.float32)
        links_ref[...] += lax.dot_general(
            links.astype(jnp.bfloat16), one_where(ids == own_item), NT, preferred_element_type=jnp.float32
        )
        total_ref[...] += links[rows:]
        return unused

    lax.fori_loop(0, blocks, block, 0, unroll=4)

    share = rows // slabs
    tail = jnp.concatenate([links_ref[rows : rows + 1], total_ref[0:1]], axis=0)
    for d in range(slabs):
        head_out[d, 0:share] = links_ref[d * share : (d + 1) * share]
        head_out[d, share : share + 2] = tail
        head_out[d, share + 2 : 8] = jnp.zeros((6 - share, LANES), jnp.float32)

    exchange(slabs, me, head_out, head_in, head_send, head_recv, True)

    def forward(k):
        far(k).wait_recv()
        near(k).start()

    each(1, slabs // 2, forward)
    exchange(slabs, me, head_out, head_in, head_send, head_recv, False)
    head_ref[...] = jnp.sum(head_in[...], axis=0)
    own_near.wait()
    each(1, slabs // 2, lambda k: near(k).wait())
    each(1, slabs // 2, lambda k: far(k).wait_send())


def take_windows(code_ref, length, start):
    whole, part = start >> 3, start & 7
    bits = max(1, (length // 8 - 1).bit_length())
    keep = 8 * ((1 << (bits - 1)) + 4)
    value = None
    for bit in reversed(range(bits)):
        step = 8 << bit
        keep = 8 * ((1 << bit) + 4)
        chosen = ((whole >> bit) & 1) == 1
        if value is None:
            low, high = code_ref[0:keep, :], code_ref[step : step + keep, :]
        else:
            low, high = value[0:keep], value[step : step + keep]
        value = jnp.where(chosen, high, low)
    for bit in (2, 1, 0):
        chosen = ((part >> bit) & 1) == 1
        value = jnp.where(chosen, pltpu.roll(value, value.shape[0] - (1 << bit), 0), value)
    return value[0:32]


def tile_kernel(rows, length, half, base_ref, all_ref, count_ref, margin_ref, flat_ref, code_ref, key_ref):
    item_mask = (1 << ITEM_BITS) - 1
    base = base_ref[0]
    count_ref[...] = jnp.zeros_like(count_ref)
    margin_ref[...] = jnp.zeros_like(margin_ref)
    band = 2 * half
    band_rows = band // LANES
    chunk = 8 * math.gcd(length // 8, 16)
    blocks = all_ref.shape[2]
    for n in range(all_ref.shape[0]):
        flat_ref[n * blocks : (n + 1) * blocks] = all_ref[n, 0] | (all_ref[n, 1] << ITEM_BITS)
    per = length // LANES
    for r in range(per):
        code_ref[16 + r * LANES : 16 + (r + 1) * LANES] = flat_ref[pl.ds(r, LANES, stride=per), :].T
    lane = lax.broadcasted_iota(jnp.int32, (16, LANES), 1)
    code_ref[0:16] = jnp.where(lane == 0, -1, pltpu.roll(code_ref[length : length + 16], 1, 1))
    code_ref[length + 16 : length + 32] = jnp.where(
        lane == LANES - 1, -1, pltpu.roll(code_ref[16:32], LANES - 1, 1)
    )

    def fill(c, tops):
        at = pl.multiple_of(c * chunk, chunk)
        item = code_ref[pl.ds(at + 16, chunk), :] & item_mask
        place = (at + lax.broadcasted_iota(jnp.int32, (chunk, LANES), 0)).astype(jnp.float32)
        new = []
        for s in range(2):
            local = item - base - s * band
            mine = (local >= 0) & (local < band) & (item >= rows)
            key_ref[s, pl.ds(at, chunk), :] = jnp.where(mine, place, BIG)
            new.append(tops[s] + jnp.sum(mine.astype(jnp.int32), axis=0, keepdims=True))
        return tuple(new)

    none = jnp.zeros((1, LANES), jnp.int32)
    tally = lax.fori_loop(0, length // chunk, fill, (none, none))
    trips = (jnp.max(jnp.maximum(tally[0], tally[1])) + 1) // 2

    row_ids = lax.broadcasted_iota(jnp.int32, (rows, 2 * LANES), 0).astype(jnp.float32)
    d_ids = lax.broadcasted_iota(jnp.int32, (32, LANES), 0)
    near = (d_ids >= 1) & (d_ids != 16)
    m_ids = lax.broadcasted_iota(jnp.int32, (max(8, band_rows), 2 * LANES), 0)
    l_ids = lax.broadcasted_iota(jnp.int32, (LANES, 2 * LANES), 0)
    tile = min(half, 512)
    t_ids = lax.broadcasted_iota(jnp.int32, (tile, 2 * LANES), 0)

    def body(unused, state):
        out = []
        for s in range(2):
            first, last = state[2 * s], state[2 * s + 1]
            key = key_ref[s]
            next_first = jnp.min(jnp.where(key > first, key, BIG), axis=0, keepdims=True)
            next_last = jnp.max(jnp.where(key < last, key, -1.0), axis=0, keepdims=True)
            first_ok = next_first < last
            last_ok = next_last > next_first
            out += [next_first, next_last]
            heads, weights, locals_ = [], [], []
            for at, ok in ((next_first, first_ok), (next_last, last_ok)):
                start = jnp.where(ok, at, 0.0).astype(jnp.int32)
                window = take_windows(code_ref, length, start)
                item, session = window & item_mask, window >> ITEM_BITS
                linked = (session == session[16:17]) & near & ok
                heads.append(jnp.where(linked & (item < rows), item, -1).astype(jnp.float32))
                weights.append(jnp.sum(jnp.where(linked, 1.0, 0.0), axis=0, keepdims=True))
                locals_.append(item[16:17] - base - s * band)
            head = jnp.concatenate(heads, axis=1)
            weight = jnp.concatenate(weights, axis=1)
            local = jnp.concatenate(locals_, axis=1)
            links = jnp.zeros((rows, 2 * LANES), jnp.float32)
            for d in range(1, 32):
                if d != 16:
                    links += jnp.where(row_ids == head[d : d + 1], 1.0, 0.0)
            upper = local >= half
            pair = jnp.concatenate(
                [jnp.where(upper, 0.0, links), jnp.where(upper, links, 0.0)], axis=0
            ).astype(jnp.bfloat16)
            inner = jnp.where(upper, local - half, local)
            for t in range(half // tile):
                hot = one_where(t_ids + t * tile == inner)
                count_ref[s, :, t * tile : (t + 1) * tile] += lax.dot_general(
                    pair, hot, NT, preferred_element_type=jnp.float32
                )
            coarse = jnp.where(m_ids == (local >> 7), weight, 0.0).astype(jnp.bfloat16)
            fine = one_where(l_ids == (local & (LANES - 1)))
            margin_ref[s] += lax.dot_general(coarse, fine, NT, preferred_element_type=jnp.float32)
        return tuple(out)

    low = jnp.full((1, LANES), -1.0, jnp.float32)
    high = jnp.full((1, LANES), BIG, jnp.float32)
    lax.fori_loop(0, trips, body, (low, high, low, high))


def sketch_kernel(
    slabs, rows, half, width, scale, count_ref, margin_ref, head_ref, bits_ref, out_ref,
    log_ref, own_bits, head_bits, acc_ref, send_ref, recv_ref, bit_sems, send_sems, recv_sems,
):
    me = lax.axis_index("stream")
    barrier = greet_all(slabs, me)
    owned = 4 * half
    share = rows // slabs
    tile = min(half, 512)
    bit_copy = pltpu.make_async_copy(
        bits_ref.at[:, pl.ds(pl.multiple_of(me * owned, owned), owned)], own_bits, bit_sems.at[0]
    )
    head_copy = pltpu.make_async_copy(bits_ref.at[:, 0:rows], head_bits, bit_sems.at[1])
    bit_copy.start()
    head_copy.start()

    log_ref[...] = jnp.log(jnp.maximum(margin_ref[...], 1.0))
    row_log = jnp.log(jnp.maximum(head_ref[share : share + 1], 1.0))
    column_log = jnp.broadcast_to(row_log, (rows, LANES)).T
    total_log = jnp.log(jnp.sum(head_ref[share + 1 : share + 2], axis=1, keepdims=True))
    row_term = total_log - column_log[:, 0:1]
    groups = []
    for g in range(width // 8):
        word = 8 * g // BITS_PER_WORD
        groups.append((word, (word + 1) * BITS_PER_WORD - 8 * g, 8 * g - word * BITS_PER_WORD))

    def product(positive, words):
        size = words.shape[1]
        shift = lax.broadcasted_iota(jnp.int32, (8, size), 0)
        upper = positive.astype(jnp.bfloat16)
        lower = (positive - upper.astype(jnp.float32)).astype(jnp.bfloat16)
        parts = []
        for word, split, offset in groups:
            now = jnp.broadcast_to(words[word : word + 1], (8, size))
            where_bit = shift + offset
            if split < 8:
                later = jnp.broadcast_to(words[word + 1 : word + 2], (8, size))
                now = jnp.where(shift >= split, later, now)
                where_bit = jnp.where(shift >= split, shift - split, where_bit)
            parts.append(jnp.where(((now >> where_bit) & 1) == 1, 1.0, -1.0))
        signs = jnp.concatenate(parts, axis=0).astype(jnp.bfloat16)
        both = jnp.concatenate([upper, lower], axis=0)
        value = lax.dot_general(both, signs, NT, preferred_element_type=jnp.float32)
        return value[0:rows] + value[rows:]

    head_copy.wait()
    row = lax.broadcasted_iota(jnp.int32, (8, LANES), 0)
    shared = jnp.concatenate(
        [jnp.where(row < share, head_ref[...], 0.0), jnp.zeros((rows - 8, LANES), jnp.float32)], axis=0
    )
    shared = pltpu.roll(shared, me * share, 0)
    ratio = jnp.log(jnp.maximum(shared, 1.0)) + total_log - row_log - column_log
    first_band = jnp.where(lax.axis_index("item") == 0, 1.0, 0.0)
    positive = jnp.where(shared > 0, jnp.maximum(ratio, 0.0), 0.0) * first_band
    acc_ref[...] = product(positive.T, head_bits[...])
    bit_copy.wait()

    for s in range(2):
        for h in range(2):

            def step(t, unused, s=s, h=h):
                at = pl.multiple_of(t * tile, tile)
                counts = count_ref[s, h * rows : (h + 1) * rows, pl.ds(at, tile)]
                first_log = h * (half // LANES) + t * (tile // LANES)
                col_log = jnp.concatenate(
                    [log_ref[s, pl.ds(first_log + n, 1), :] for n in range(tile // LANES)], axis=1
                )
                ratio = jnp.log(jnp.maximum(counts, 1.0)) + row_term - col_log
                positive = jnp.where(counts > 0, jnp.maximum(ratio, 0.0), 0.0)
                bit_at = pl.multiple_of(s * 2 * half + h * half + t * tile, tile)
                acc_ref[...] += product(positive, own_bits[:, pl.ds(bit_at, tile)])
                return unused

            lax.fori_loop(0, half // tile, step, 0)

    cuts = width // LANES
    for d in range(slabs):
        for c in range(cuts):
            send_ref[d, c * share : (c + 1) * share] = (
                acc_ref[d * share : (d + 1) * share, c * LANES : (c + 1) * LANES] * scale
            )
    pl.semaphore_wait(barrier, slabs - 1)
    exchange(slabs, me, send_ref, recv_ref, send_sems, recv_sems, True)
    exchange(slabs, me, send_ref, recv_ref, send_sems, recv_sems, False)
    summed = jnp.sum(recv_ref[...], axis=0)
    out_ref[...] = jnp.concatenate([summed[c * share : (c + 1) * share] for c in range(cuts)], axis=1)


def local(event_items, event_sessions, sketch_bits):
    slabs = lax.axis_size("stream")
    slab = event_items.shape[0]
    total_events = slab * slabs
    words, band_size = sketch_bits.shape
    owned = band_size // slabs
    rows, width, half = 128, 256, owned // 4
    me = lax.axis_index("stream")
    own_start = me * owned
    first_id = lax.axis_index("item") * band_size + own_start
    blocks = slab // LANES
    length = total_events // LANES

    stacked = jnp.stack([event_items, event_sessions]).reshape(2, blocks, LANES)
    dma = pltpu.SemaphoreType.DMA
    events, head = pl.pallas_call(
        functools.partial(gather_kernel, slabs, rows, blocks),
        out_shape=(
            jax.ShapeDtypeStruct((slabs, 2, blocks, LANES), jnp.int32),
            jax.ShapeDtypeStruct((8, LANES), jnp.float32),
        ),
        in_specs=[VMEM],
        out_specs=(VMEM, VMEM),
        scratch_shapes=[
            pltpu.VMEM((2, 2, 8, LANES), jnp.int32),
            pltpu.VMEM((blocks + 16, LANES), jnp.int32),
            pltpu.VMEM((blocks + 16, LANES), jnp.int32),
            pltpu.VMEM((rows + 8, LANES), jnp.float32),
            pltpu.VMEM((8, LANES), jnp.float32),
            pltpu.VMEM((slabs, 8, LANES), jnp.float32),
            pltpu.VMEM((slabs, 8, LANES), jnp.float32),
            dma((slabs // 2,)),
            dma((slabs // 2,)),
            dma((slabs // 2,)),
            dma((slabs // 2,)),
            dma((2,)),
            dma((2,)),
            dma((slabs,)),
            dma((slabs,)),
        ],
        compiler_params=pltpu.CompilerParams(collective_id=0, has_side_effects=True),
        name="gather_events",
    )(stacked)

    band_rows = max(8, 2 * half // LANES)
    counts, margins = pl.pallas_call(
        functools.partial(tile_kernel, rows, length, half),
        out_shape=(
            jax.ShapeDtypeStruct((2, 2 * rows, half), jnp.float32),
            jax.ShapeDtypeStruct((2, band_rows, LANES), jnp.float32),
        ),
        in_specs=[pl.BlockSpec(memory_space=pltpu.SMEM), VMEM],
        out_specs=(VMEM, VMEM),
        scratch_shapes=[
            pltpu.VMEM((length, LANES), jnp.int32),
            pltpu.VMEM((length + 32, LANES), jnp.int32),
            pltpu.VMEM((2, length, LANES), jnp.float32),
        ],
        name="tile_counts",
    )(first_id.astype(jnp.int32)[None], events)

    own_rows = pl.pallas_call(
        functools.partial(sketch_kernel, slabs, rows, half, width, 1.0 / math.sqrt(total_events)),
        out_shape=jax.ShapeDtypeStruct((rows // slabs, width), jnp.float32),
        in_specs=[VMEM] * 3 + [pl.BlockSpec(memory_space=pl.ANY)],
        out_specs=VMEM,
        scratch_shapes=[
            pltpu.VMEM((2, band_rows, LANES), jnp.float32),
            pltpu.VMEM((words, owned), jnp.int32),
            pltpu.VMEM((words, rows), jnp.int32),
            pltpu.VMEM((rows, width), jnp.float32),
            pltpu.VMEM((slabs, 8, LANES), jnp.float32),
            pltpu.VMEM((slabs, 8, LANES), jnp.float32),
            dma((2,)),
            dma((slabs,)),
            dma((slabs,)),
        ],
        compiler_params=pltpu.CompilerParams(collective_id=1, has_side_effects=True),
        name="sketch_tile",
    )(counts, margins, head, sketch_bits)
    if lax.axis_size("item") > 1:
        own_rows = lax.psum(own_rows, "item")
    return own_rows


def solution(mesh):
    placed = (P("stream"), P("stream"), P(None, "item"))
    return jax.shard_map(
        local, mesh=mesh, in_specs=placed, out_specs=P("stream", None), check_vma=False
    )
```

```python
import functools
import math

import jax
import jax.numpy as jnp
from jax import lax
from jax.experimental import pallas as pl
from jax.experimental.pallas import tpu as pltpu
from jax.sharding import PartitionSpec as P

WINDOW = 15
ITEM_BITS = 18
LANES = 128
BITS_PER_WORD = 18
BIG = 1.0e6
VMEM_GRANT = 50 * 1024 * 1024
NT = (((1,), (1,)), ((), ()))
VMEM = pl.BlockSpec(memory_space=pltpu.VMEM)


def one_where(mask):
    return jnp.where(mask, 1.0, 0.0).astype(jnp.bfloat16)


def hot_columns(ids, values):
    row = jnp.broadcast_to(values, (16, values.shape[1])).astype(jnp.bfloat16)
    one, zero = jnp.ones((), jnp.bfloat16), jnp.zeros((), jnp.bfloat16)
    return jnp.concatenate(
        [jnp.where(ids[n : n + 16] == row, one, zero) for n in range(0, ids.shape[0], 16)], axis=0
    )


def greet_all(slabs, me):
    barrier = pltpu.get_barrier_semaphore()

    def signal(k, unused):
        pl.semaphore_signal(
            barrier, inc=1, device_id={"stream": lax.rem(me + k, slabs)}, device_id_type=pl.DeviceIdType.MESH
        )
        return unused

    lax.fori_loop(1, slabs, signal, 0)
    return barrier


def send(src, dst, send_sem, recv_sem, to):
    return pltpu.make_async_remote_copy(
        src_ref=src,
        dst_ref=dst,
        send_sem=send_sem,
        recv_sem=recv_sem,
        device_id={"stream": to},
        device_id_type=pl.DeviceIdType.MESH,
    )


def each(low, high, do):
    def step(k, unused):
        do(k)
        return unused

    lax.fori_loop(low, high, step, 0)


def exchange(slabs, me, out_ref, in_ref, send_sems, recv_sems, start):
    def copy(k):
        to = lax.rem(me + k, slabs)
        return send(out_ref.at[to], in_ref.at[me], send_sems.at[k], recv_sems.at[k], to)

    if start:
        each(1, slabs, lambda k: copy(k).start())
        in_ref[me] = out_ref[me]
    else:
        each(1, slabs, lambda k: copy(k).wait())


def gather_kernel(
    slabs, rows, blocks, own_ref, all_ref, head_ref, halo_ref, item_ref, session_ref, links_ref, total_ref,
    head_out, head_in, far_send, far_recv, near_send, near_recv, halo_send, halo_recv, head_send, head_recv,
):
    me = lax.axis_index("stream")
    partner = me + 1 - 2 * lax.rem(me, 2)
    after, before = lax.rem(me + 1, slabs), lax.rem(me + slabs - 1, slabs)
    barrier = greet_all(slabs, me)
    pl.semaphore_wait(barrier, slabs - 1)

    low_halo = send(own_ref.at[:, blocks - 8 : blocks], halo_ref.at[0], halo_send.at[0], halo_recv.at[0], after)
    high_halo = send(own_ref.at[:, 0:8], halo_ref.at[1], halo_send.at[1], halo_recv.at[1], before)
    low_halo.start()
    high_halo.start()

    def far(k):
        return send(own_ref, all_ref.at[me], far_send.at[k], far_recv.at[k], lax.rem(me + 2 * k, slabs))

    def near(k):
        source = lax.rem(me + 2 * slabs - 2 * k, slabs)
        return send(all_ref.at[source], all_ref.at[source], near_send.at[k], near_recv.at[k], partner)

    own_near = send(own_ref, all_ref.at[me], near_send.at[0], near_recv.at[0], partner)
    own_near.start()
    each(1, slabs // 2, lambda k: far(k).start())
    all_ref[me] = own_ref[...]

    item_ref[8 : 8 + blocks] = own_ref[0]
    session_ref[8 : 8 + blocks] = own_ref[1]
    low_halo.wait()
    high_halo.wait()
    item_ref[0:8] = halo_ref[0, 0]
    item_ref[8 + blocks : 16 + blocks] = halo_ref[1, 0]
    session_ref[0:8] = jnp.where(me == 0, -1, halo_ref[0, 1])
    session_ref[8 + blocks : 16 + blocks] = jnp.where(me == slabs - 1, -1, halo_ref[1, 1])

    sub = lax.broadcasted_iota(jnp.int32, (LANES, LANES), 0)
    lane = lax.broadcasted_iota(jnp.int32, (LANES, LANES), 1)
    low_lane = lax.broadcasted_iota(jnp.int32, (1, LANES), 1) < LANES // 2
    ids = lax.broadcasted_iota(jnp.int32, (rows, LANES), 0)
    gaps = (sub - LANES // 2 - lane, sub + LANES // 2 - lane)
    in_reach = [(jnp.abs(gap) <= WINDOW) & (gap != 0) for gap in gaps]
    ones = jnp.ones((8, 2 * LANES), jnp.float32).astype(jnp.bfloat16)
    links_ref[...] = jnp.zeros_like(links_ref)
    total_ref[...] = jnp.zeros_like(total_ref)

    def block(b, unused):
        def around(ref):
            turned = [pltpu.roll(ref[pl.ds(b + o, 1)], LANES // 2, 1) for o in (7, 8, 9)]
            return (
                jnp.where(low_lane, turned[0], turned[1]),
                jnp.where(low_lane, turned[1], turned[2]),
            )

        own_item, own_session = item_ref[pl.ds(b + 8, 1)], session_ref[pl.ds(b + 8, 1)]
        hot = jnp.concatenate([one_where(ids == item) for item in around(item_ref)], axis=1)
        linked = jnp.concatenate(
            [
                one_where((jnp.broadcast_to(session, (LANES, LANES)).T == own_session) & reach)
                for session, reach in zip(around(session_ref), in_reach)
            ],
            axis=0,
        )
        links = jnp.dot(jnp.concatenate([hot, ones], axis=0), linked, preferred_element_type=jnp.float32)
        links_ref[...] += lax.dot_general(
            links.astype(jnp.bfloat16), one_where(ids == own_item), NT, preferred_element_type=jnp.float32
        )
        total_ref[...] += links[rows:]
        return unused

    lax.fori_loop(0, blocks, block, 0, unroll=4)

    share = rows // slabs
    tail = jnp.concatenate([links_ref[rows : rows + 1], total_ref[0:1]], axis=0)
    for d in range(slabs):
        head_out[d, 0:share] = links_ref[d * share : (d + 1) * share]
        head_out[d, share : share + 2] = tail
        head_out[d, share + 2 : 8] = jnp.zeros((6 - share, LANES), jnp.float32)

    exchange(slabs, me, head_out, head_in, head_send, head_recv, True)

    def forward(k):
        far(k).wait_recv()
        near(k).start()

    each(1, slabs // 2, forward)
    exchange(slabs, me, head_out, head_in, head_send, head_recv, False)
    head_ref[...] = jnp.sum(head_in[...], axis=0)
    own_near.wait()
    each(1, slabs // 2, lambda k: near(k).wait())
    each(1, slabs // 2, lambda k: far(k).wait_send())


def take_windows(code_ref, length, start):
    whole, part = start >> 3, start & 7
    bits = max(1, (length // 8 - 1).bit_length())
    keep = 8 * ((1 << (bits - 1)) + 4)
    value = None
    for bit in reversed(range(bits)):
        step = 8 << bit
        keep = 8 * ((1 << bit) + 4)
        chosen = ((whole >> bit) & 1) == 1
        if value is None:
            low, high = code_ref[0:keep, :], code_ref[step : step + keep, :]
        else:
            low, high = value[0:keep], value[step : step + keep]
        value = jnp.where(chosen, high, low)
    for bit in (2, 1, 0):
        chosen = ((part >> bit) & 1) == 1
        value = jnp.where(chosen, pltpu.roll(value, value.shape[0] - (1 << bit), 0), value)
    return value[0:32]


def tile_kernel(rows, length, half, base_ref, all_ref, count_ref, margin_ref, flat_ref, code_ref, key_ref):
    item_mask = (1 << ITEM_BITS) - 1
    base = base_ref[0]
    count_ref[...] = jnp.zeros_like(count_ref)
    margin_ref[...] = jnp.zeros_like(margin_ref)
    band = 2 * half
    band_rows = band // LANES
    chunk = 8 * math.gcd(length // 8, 16)
    blocks = all_ref.shape[2]
    for n in range(all_ref.shape[0]):
        flat_ref[n * blocks : (n + 1) * blocks] = all_ref[n, 0] | (all_ref[n, 1] << ITEM_BITS)
    per = length // LANES
    for r in range(per):
        code_ref[16 + r * LANES : 16 + (r + 1) * LANES] = flat_ref[pl.ds(r, LANES, stride=per), :].T
    lane = lax.broadcasted_iota(jnp.int32, (16, LANES), 1)
    code_ref[0:16] = jnp.where(lane == 0, -1, pltpu.roll(code_ref[length : length + 16], 1, 1))
    code_ref[length + 16 : length + 32] = jnp.where(
        lane == LANES - 1, -1, pltpu.roll(code_ref[16:32], LANES - 1, 1)
    )

    def fill(c, tops):
        at = pl.multiple_of(c * chunk, chunk)
        item = code_ref[pl.ds(at + 16, chunk), :] & item_mask
        place = (at + lax.broadcasted_iota(jnp.int32, (chunk, LANES), 0)).astype(jnp.float32)
        new = []
        for s in range(2):
            local = item - base - s * band
            mine = (local >= 0) & (local < band) & (item >= rows)
            key_ref[s, pl.ds(at, chunk), :] = jnp.where(mine, place, BIG)
            new.append(tops[s] + jnp.sum(mine.astype(jnp.int32), axis=0, keepdims=True))
        return tuple(new)

    none = jnp.zeros((1, LANES), jnp.int32)
    tally = lax.fori_loop(0, length // chunk, fill, (none, none))
    trips = (jnp.max(jnp.maximum(tally[0], tally[1])) + 1) // 2

    row_ids = lax.broadcasted_iota(jnp.int32, (rows, 2 * LANES), 0).astype(jnp.float32).astype(jnp.bfloat16)
    d_ids = lax.broadcasted_iota(jnp.int32, (32, LANES), 0)
    near = (d_ids >= 1) & (d_ids != 16)
    m_ids = lax.broadcasted_iota(jnp.int32, (max(8, band_rows), 2 * LANES), 0)
    l_ids = lax.broadcasted_iota(jnp.int32, (LANES, 2 * LANES), 0)
    tile = 256
    t_ids = lax.broadcasted_iota(jnp.int32, (tile, 2 * LANES), 0).astype(jnp.float32).astype(jnp.bfloat16)

    def body(unused, state):
        out = []
        for s in range(2):
            first, last = state[2 * s], state[2 * s + 1]
            key = key_ref[s]
            next_first = jnp.min(jnp.where(key > first, key, BIG), axis=0, keepdims=True)
            next_last = jnp.max(jnp.where(key < last, key, -1.0), axis=0, keepdims=True)
            first_ok = next_first < last
            last_ok = next_last > next_first
            out += [next_first, next_last]
            heads, weights, locals_ = [], [], []
            for at, ok in ((next_first, first_ok), (next_last, last_ok)):
                start = jnp.where(ok, at, 0.0).astype(jnp.int32)
                window = take_windows(code_ref, length, start)
                item, session = window & item_mask, window >> ITEM_BITS
                linked = (session == session[16:17]) & near & ok
                heads.append(jnp.where(linked & (item < rows), item, -1).astype(jnp.float32))
                weights.append(jnp.sum(jnp.where(linked, 1.0, 0.0), axis=0, keepdims=True))
                locals_.append(item[16:17] - base - s * band)
            head = jnp.concatenate(heads, axis=1)
            weight = jnp.concatenate(weights, axis=1)
            local = jnp.concatenate(locals_, axis=1)
            links = jnp.zeros((rows, 2 * LANES), jnp.bfloat16)
            for d in range(1, 32):
                if d != 16:
                    links += hot_columns(row_ids, head[d : d + 1])
            upper = local >= half
            side = jnp.broadcast_to(jnp.where(upper, 1.0, 0.0), (16, 2 * LANES)).astype(jnp.bfloat16)
            high_part = jnp.concatenate([links[n : n + 16] * side for n in range(0, rows, 16)], axis=0)
            pair = jnp.concatenate([links - high_part, high_part], axis=0)
            inner = jnp.where(upper, local - half, local)
            for t in range(half // tile):
                inside = (inner >= t * tile) & (inner < (t + 1) * tile)
                hot = hot_columns(t_ids, jnp.where(inside, inner - t * tile, -1).astype(jnp.float32))
                count_ref[s, :, t * tile : (t + 1) * tile] += lax.dot_general(
                    pair, hot, NT, preferred_element_type=jnp.float32
                )
            coarse = jnp.where(m_ids == (local >> 7), weight, 0.0).astype(jnp.bfloat16)
            fine = one_where(l_ids == (local & (LANES - 1)))
            margin_ref[s] += lax.dot_general(coarse, fine, NT, preferred_element_type=jnp.float32)
        return tuple(out)

    low = jnp.full((1, LANES), -1.0, jnp.float32)
    high = jnp.full((1, LANES), BIG, jnp.float32)
    lax.fori_loop(0, trips, body, (low, high, low, high))


def sketch_kernel(
    slabs, rows, half, width, scale, count_ref, margin_ref, head_ref, bits_ref, out_ref,
    log_ref, own_bits, head_bits, acc_ref, send_ref, recv_ref, bit_sems, send_sems, recv_sems,
):
    me = lax.axis_index("stream")
    barrier = greet_all(slabs, me)
    owned = 4 * half
    share = rows // slabs
    tile = min(half, 512)
    bit_copy = pltpu.make_async_copy(
        bits_ref.at[:, pl.ds(pl.multiple_of(me * owned, owned), owned)], own_bits, bit_sems.at[0]
    )
    head_copy = pltpu.make_async_copy(bits_ref.at[:, 0:rows], head_bits, bit_sems.at[1])
    bit_copy.start()
    head_copy.start()

    log_ref[...] = jnp.log(jnp.maximum(margin_ref[...], 1.0))
    row_log = jnp.log(jnp.maximum(head_ref[share : share + 1], 1.0))
    column_log = jnp.broadcast_to(row_log, (rows, LANES)).T
    total_log = jnp.log(jnp.sum(head_ref[share + 1 : share + 2], axis=1, keepdims=True))
    row_term = total_log - column_log[:, 0:1]
    groups = []
    for g in range(width // 8):
        word = 8 * g // BITS_PER_WORD
        groups.append((word, (word + 1) * BITS_PER_WORD - 8 * g, 8 * g - word * BITS_PER_WORD))

    def product(positive, words):
        size = words.shape[1]
        shift = lax.broadcasted_iota(jnp.int32, (8, size), 0)
        upper = positive.astype(jnp.bfloat16)
        lower = (positive - upper.astype(jnp.float32)).astype(jnp.bfloat16)
        parts = []
        for word, split, offset in groups:
            now = jnp.broadcast_to(words[word : word + 1], (8, size))
            where_bit = shift + offset
            if split < 8:
                later = jnp.broadcast_to(words[word + 1 : word + 2], (8, size))
                now = jnp.where(shift >= split, later, now)
                where_bit = jnp.where(shift >= split, shift - split, where_bit)
            parts.append(jnp.where(((now >> where_bit) & 1) == 1, 1.0, -1.0))
        signs = jnp.concatenate(parts, axis=0).astype(jnp.bfloat16)
        both = jnp.concatenate([upper, lower], axis=0)
        value = lax.dot_general(both, signs, NT, preferred_element_type=jnp.float32)
        return value[0:rows] + value[rows:]

    head_copy.wait()
    row = lax.broadcasted_iota(jnp.int32, (8, LANES), 0)
    shared = jnp.concatenate(
        [jnp.where(row < share, head_ref[...], 0.0), jnp.zeros((rows - 8, LANES), jnp.float32)], axis=0
    )
    shared = pltpu.roll(shared, me * share, 0)
    ratio = jnp.log(jnp.maximum(shared, 1.0)) + total_log - row_log - column_log
    first_band = jnp.where(lax.axis_index("item") == 0, 1.0, 0.0)
    positive = jnp.where(shared > 0, jnp.maximum(ratio, 0.0), 0.0) * first_band
    acc_ref[...] = product(positive.T, head_bits[...])
    bit_copy.wait()

    for s in range(2):
        for h in range(2):

            def step(t, unused, s=s, h=h):
                at = pl.multiple_of(t * tile, tile)
                counts = count_ref[s, h * rows : (h + 1) * rows, pl.ds(at, tile)]
                first_log = h * (half // LANES) + t * (tile // LANES)
                col_log = jnp.concatenate(
                    [log_ref[s, pl.ds(first_log + n, 1), :] for n in range(tile // LANES)], axis=1
                )
                ratio = jnp.log(jnp.maximum(counts, 1.0)) + row_term - col_log
                positive = jnp.where(counts > 0, jnp.maximum(ratio, 0.0), 0.0)
                bit_at = pl.multiple_of(s * 2 * half + h * half + t * tile, tile)
                acc_ref[...] += product(positive, own_bits[:, pl.ds(bit_at, tile)])
                return unused

            lax.fori_loop(0, half // tile, step, 0)

    cuts = width // LANES
    for d in range(slabs):
        for c in range(cuts):
            send_ref[d, c * share : (c + 1) * share] = (
                acc_ref[d * share : (d + 1) * share, c * LANES : (c + 1) * LANES] * scale
            )
    pl.semaphore_wait(barrier, slabs - 1)
    exchange(slabs, me, send_ref, recv_ref, send_sems, recv_sems, True)
    exchange(slabs, me, send_ref, recv_ref, send_sems, recv_sems, False)
    summed = jnp.sum(recv_ref[...], axis=0)
    out_ref[...] = jnp.concatenate([summed[c * share : (c + 1) * share] for c in range(cuts)], axis=1)


def local(event_items, event_sessions, sketch_bits):
    slabs = lax.axis_size("stream")
    slab = event_items.shape[0]
    total_events = slab * slabs
    words, band_size = sketch_bits.shape
    owned = band_size // slabs
    rows, width, half = 128, 256, owned // 4
    me = lax.axis_index("stream")
    own_start = me * owned
    first_id = lax.axis_index("item") * band_size + own_start
    blocks = slab // LANES
    length = total_events // LANES

    stacked = jnp.stack([event_items, event_sessions]).reshape(2, blocks, LANES)
    dma = pltpu.SemaphoreType.DMA
    events, head = pl.pallas_call(
        functools.partial(gather_kernel, slabs, rows, blocks),
        out_shape=(
            jax.ShapeDtypeStruct((slabs, 2, blocks, LANES), jnp.int32),
            jax.ShapeDtypeStruct((8, LANES), jnp.float32),
        ),
        in_specs=[VMEM],
        out_specs=(VMEM, VMEM),
        scratch_shapes=[
            pltpu.VMEM((2, 2, 8, LANES), jnp.int32),
            pltpu.VMEM((blocks + 16, LANES), jnp.int32),
            pltpu.VMEM((blocks + 16, LANES), jnp.int32),
            pltpu.VMEM((rows + 8, LANES), jnp.float32),
            pltpu.VMEM((8, LANES), jnp.float32),
            pltpu.VMEM((slabs, 8, LANES), jnp.float32),
            pltpu.VMEM((slabs, 8, LANES), jnp.float32),
            dma((slabs // 2,)),
            dma((slabs // 2,)),
            dma((slabs // 2,)),
            dma((slabs // 2,)),
            dma((2,)),
            dma((2,)),
            dma((slabs,)),
            dma((slabs,)),
        ],
        compiler_params=pltpu.CompilerParams(
            collective_id=0, has_side_effects=True, vmem_limit_bytes=VMEM_GRANT
        ),
        name="gather_events",
    )(stacked)

    band_rows = max(8, 2 * half // LANES)
    counts, margins = pl.pallas_call(
        functools.partial(tile_kernel, rows, length, half),
        out_shape=(
            jax.ShapeDtypeStruct((2, 2 * rows, half), jnp.float32),
            jax.ShapeDtypeStruct((2, band_rows, LANES), jnp.float32),
        ),
        in_specs=[pl.BlockSpec(memory_space=pltpu.SMEM), VMEM],
        out_specs=(VMEM, VMEM),
        scratch_shapes=[
            pltpu.VMEM((length, LANES), jnp.int32),
            pltpu.VMEM((length + 32, LANES), jnp.int32),
            pltpu.VMEM((2, length, LANES), jnp.float32),
        ],
        compiler_params=pltpu.CompilerParams(vmem_limit_bytes=VMEM_GRANT),
        name="tile_counts",
    )(first_id.astype(jnp.int32)[None], events)

    own_rows = pl.pallas_call(
        functools.partial(sketch_kernel, slabs, rows, half, width, 1.0 / math.sqrt(total_events)),
        out_shape=jax.ShapeDtypeStruct((rows // slabs, width), jnp.float32),
        in_specs=[VMEM] * 3 + [pl.BlockSpec(memory_space=pl.ANY)],
        out_specs=VMEM,
        scratch_shapes=[
            pltpu.VMEM((2, band_rows, LANES), jnp.float32),
            pltpu.VMEM((words, owned), jnp.int32),
            pltpu.VMEM((words, rows), jnp.int32),
            pltpu.VMEM((rows, width), jnp.float32),
            pltpu.VMEM((slabs, 8, LANES), jnp.float32),
            pltpu.VMEM((slabs, 8, LANES), jnp.float32),
            dma((2,)),
            dma((slabs,)),
            dma((slabs,)),
        ],
        compiler_params=pltpu.CompilerParams(
            collective_id=1, has_side_effects=True, vmem_limit_bytes=VMEM_GRANT
        ),
        name="sketch_tile",
    )(counts, margins, head, sketch_bits)
    if lax.axis_size("item") > 1:
        own_rows = lax.psum(own_rows, "item")
    return own_rows


def solution(mesh):
    placed = (P("stream"), P("stream"), P(None, "item"))
    return jax.shard_map(
        local, mesh=mesh, in_specs=placed, out_specs=P("stream", None), check_vma=False
    )
```

```python
import functools
import math

import jax
import jax.numpy as jnp
from jax import lax
from jax.experimental import pallas as pl
from jax.experimental.pallas import tpu as pltpu
from jax.sharding import PartitionSpec as P

WINDOW = 15
ITEM_BITS = 18
LANES = 128
BITS_PER_WORD = 18
BIG = 1.0e6
VMEM_GRANT = 45 * 1024 * 1024
NT = (((1,), (1,)), ((), ()))
VMEM = pl.BlockSpec(memory_space=pltpu.VMEM)


def one_where(mask):
    return jnp.where(mask, 1.0, 0.0).astype(jnp.bfloat16)


def hot_columns(ids, values):
    row = jnp.broadcast_to(values, (16, values.shape[1])).astype(jnp.bfloat16)
    one, zero = jnp.ones((), jnp.bfloat16), jnp.zeros((), jnp.bfloat16)
    return jnp.concatenate(
        [jnp.where(ids[n : n + 16] == row, one, zero) for n in range(0, ids.shape[0], 16)], axis=0
    )


def greet_all(slabs, me):
    barrier = pltpu.get_barrier_semaphore()

    def signal(k, unused):
        pl.semaphore_signal(
            barrier, inc=1, device_id={"stream": lax.rem(me + k, slabs)}, device_id_type=pl.DeviceIdType.MESH
        )
        return unused

    lax.fori_loop(1, slabs, signal, 0)
    return barrier


def send(src, dst, send_sem, recv_sem, to):
    return pltpu.make_async_remote_copy(
        src_ref=src,
        dst_ref=dst,
        send_sem=send_sem,
        recv_sem=recv_sem,
        device_id={"stream": to},
        device_id_type=pl.DeviceIdType.MESH,
    )


def each(low, high, do):
    def step(k, unused):
        do(k)
        return unused

    lax.fori_loop(low, high, step, 0)


def exchange(slabs, me, out_ref, in_ref, send_sems, recv_sems, start):
    def copy(k):
        to = lax.rem(me + k, slabs)
        return send(out_ref.at[to], in_ref.at[me], send_sems.at[k], recv_sems.at[k], to)

    if start:
        each(1, slabs, lambda k: copy(k).start())
        in_ref[me] = out_ref[me]
    else:
        each(1, slabs, lambda k: copy(k).wait())


def gather_kernel(
    slabs, rows, blocks, own_items, own_sessions, all_items, all_sessions, head_ref,
    short_ref, halo_ref, item_ref, session_ref, links_ref, total_ref,
    head_out, head_in, far_send, far_recv, near_send, near_recv, halo_send, halo_recv, head_send, head_recv,
):
    me = lax.axis_index("stream")
    partner = me + 1 - 2 * lax.rem(me, 2)
    after, before = lax.rem(me + 1, slabs), lax.rem(me + slabs - 1, slabs)
    barrier = greet_all(slabs, me)
    short_ref[...] = own_sessions[...].astype(jnp.int16)
    item_ref[8 : 8 + blocks] = own_items[...]
    session_ref[8 : 8 + blocks] = own_sessions[...]
    all_items[me] = own_items[...]
    all_sessions[me] = short_ref[...]
    pl.semaphore_wait(barrier, slabs - 1)

    halos = []
    for n, ref in enumerate((own_items, own_sessions)):
        for side, to, rows_sent in ((0, after, ref.at[blocks - 8 : blocks]), (1, before, ref.at[0:8])):
            at = 2 * n + side
            halos.append(send(rows_sent, halo_ref.at[at], halo_send.at[at], halo_recv.at[at], to))
    for copy in halos:
        copy.start()

    pairs = ((own_items, all_items, 0), (short_ref, all_sessions, slabs // 2))

    def far(k):
        to = lax.rem(me + 2 * k, slabs)
        return [
            send(own, every.at[me], far_send.at[at + k], far_recv.at[at + k], to) for own, every, at in pairs
        ]

    def near(k):
        source = lax.rem(me + 2 * slabs - 2 * k, slabs)
        return [
            send(every.at[source], every.at[source], near_send.at[at + k], near_recv.at[at + k], partner)
            for own, every, at in pairs
        ]

    def do_all(copies, act):
        for copy in copies:
            act(copy)

    own_near = [
        send(own, every.at[me], near_send.at[at], near_recv.at[at], partner) for own, every, at in pairs
    ]
    each(1, slabs // 2, lambda k: do_all(far(k), lambda c: c.start()))
    do_all(own_near, lambda c: c.start())

    sub = lax.broadcasted_iota(jnp.int32, (LANES, LANES), 0)
    lane = lax.broadcasted_iota(jnp.int32, (LANES, LANES), 1)
    low_lane = lax.broadcasted_iota(jnp.int32, (1, LANES), 1) < LANES // 2
    ids = lax.broadcasted_iota(jnp.int32, (rows, LANES), 0)
    gaps = (sub - LANES // 2 - lane, sub + LANES // 2 - lane)
    in_reach = [(jnp.abs(gap) <= WINDOW) & (gap != 0) for gap in gaps]
    ones = jnp.ones((8, 2 * LANES), jnp.float32).astype(jnp.bfloat16)
    links_ref[...] = jnp.zeros_like(links_ref)
    total_ref[...] = jnp.zeros_like(total_ref)

    def block(b, unused):
        def around(ref):
            turned = [pltpu.roll(ref[pl.ds(b + o, 1)], LANES // 2, 1) for o in (7, 8, 9)]
            return (
                jnp.where(low_lane, turned[0], turned[1]),
                jnp.where(low_lane, turned[1], turned[2]),
            )

        own_item, own_session = item_ref[pl.ds(b + 8, 1)], session_ref[pl.ds(b + 8, 1)]
        hot = jnp.concatenate([one_where(ids == item) for item in around(item_ref)], axis=1)
        linked = jnp.concatenate(
            [
                one_where((jnp.broadcast_to(session, (LANES, LANES)).T == own_session) & reach)
                for session, reach in zip(around(session_ref), in_reach)
            ],
            axis=0,
        )
        links = jnp.dot(jnp.concatenate([hot, ones], axis=0), linked, preferred_element_type=jnp.float32)
        links_ref[...] += lax.dot_general(
            links.astype(jnp.bfloat16), one_where(ids == own_item), NT, preferred_element_type=jnp.float32
        )
        total_ref[...] += links[rows:]
        return unused

    lax.fori_loop(1, blocks - 1, block, 0, unroll=5)
    for copy in halos:
        copy.wait()
    item_ref[0:8] = halo_ref[0]
    item_ref[8 + blocks : 16 + blocks] = halo_ref[1]
    session_ref[0:8] = jnp.where(me == 0, -1, halo_ref[2])
    session_ref[8 + blocks : 16 + blocks] = jnp.where(me == slabs - 1, -1, halo_ref[3])
    block(0, 0)
    block(blocks - 1, 0)

    share = rows // slabs
    tail = jnp.concatenate([links_ref[rows : rows + 1], total_ref[0:1]], axis=0)
    for d in range(slabs):
        head_out[d, 0:share] = links_ref[d * share : (d + 1) * share]
        head_out[d, share : share + 2] = tail
        head_out[d, share + 2 : 8] = jnp.zeros((6 - share, LANES), jnp.float32)

    exchange(slabs, me, head_out, head_in, head_send, head_recv, True)

    def forward(k):
        do_all(far(k), lambda c: c.wait_recv())
        do_all(near(k), lambda c: c.start())

    each(1, slabs // 2, forward)
    exchange(slabs, me, head_out, head_in, head_send, head_recv, False)
    head_ref[...] = jnp.sum(head_in[...], axis=0)
    do_all(own_near, lambda c: c.wait())
    each(1, slabs // 2, lambda k: do_all(near(k), lambda c: c.wait()))
    each(1, slabs // 2, lambda k: do_all(far(k), lambda c: c.wait_send()))


def take_windows(code_ref, length, start):
    whole, part = start >> 3, start & 7
    bits = max(1, (length // 8 - 1).bit_length())
    keep = 8 * ((1 << (bits - 1)) + 4)
    value = None
    for bit in reversed(range(bits)):
        step = 8 << bit
        keep = 8 * ((1 << bit) + 4)
        chosen = ((whole >> bit) & 1) == 1
        if value is None:
            low, high = code_ref[0:keep, :], code_ref[step : step + keep, :]
        else:
            low, high = value[0:keep], value[step : step + keep]
        value = jnp.where(chosen, high, low)
    for bit in (2, 1, 0):
        chosen = ((part >> bit) & 1) == 1
        value = jnp.where(chosen, pltpu.roll(value, value.shape[0] - (1 << bit), 0), value)
    return value[0:32]


def tile_kernel(rows, length, half, base_ref, all_items, all_sessions, count_ref, margin_ref, flat_ref, code_ref, key_ref):
    item_mask = (1 << ITEM_BITS) - 1
    base = base_ref[0]
    count_ref[...] = jnp.zeros_like(count_ref)
    margin_ref[...] = jnp.zeros_like(margin_ref)
    band = 2 * half
    band_rows = band // LANES
    chunk = 8 * math.gcd(length // 8, 16)
    slabs, blocks, unused_lanes = all_items.shape
    for n in range(slabs):
        flat_ref[n * blocks : (n + 1) * blocks] = all_items[n] | (all_sessions[n].astype(jnp.int32) << ITEM_BITS)
    per = length // LANES
    for r in range(per):
        code_ref[16 + r * LANES : 16 + (r + 1) * LANES] = flat_ref[pl.ds(r, LANES, stride=per), :].T
    lane = lax.broadcasted_iota(jnp.int32, (16, LANES), 1)
    code_ref[0:16] = jnp.where(lane == 0, -1, pltpu.roll(code_ref[length : length + 16], 1, 1))
    code_ref[length + 16 : length + 32] = jnp.where(
        lane == LANES - 1, -1, pltpu.roll(code_ref[16:32], LANES - 1, 1)
    )

    def fill(c, tops):
        at = pl.multiple_of(c * chunk, chunk)
        item = code_ref[pl.ds(at + 16, chunk), :] & item_mask
        place = (at + lax.broadcasted_iota(jnp.int32, (chunk, LANES), 0)).astype(jnp.float32)
        new = []
        for s in range(2):
            local = item - base - s * band
            mine = (local >= 0) & (local < band) & (item >= rows)
            key_ref[s, pl.ds(at, chunk), :] = jnp.where(mine, place, BIG)
            new.append(tops[s] + jnp.sum(mine.astype(jnp.int32), axis=0, keepdims=True))
        return tuple(new)

    none = jnp.zeros((1, LANES), jnp.int32)
    tally = lax.fori_loop(0, length // chunk, fill, (none, none))
    trips = (jnp.max(jnp.maximum(tally[0], tally[1])) + 1) // 2

    row_ids = lax.broadcasted_iota(jnp.int32, (rows, 2 * LANES), 0).astype(jnp.float32).astype(jnp.bfloat16)
    d_ids = lax.broadcasted_iota(jnp.int32, (32, LANES), 0)
    near = (d_ids >= 1) & (d_ids != 16)
    m_ids = lax.broadcasted_iota(jnp.int32, (max(8, band_rows), 2 * LANES), 0)
    l_ids = lax.broadcasted_iota(jnp.int32, (LANES, 2 * LANES), 0)
    tile = 256
    t_ids = lax.broadcasted_iota(jnp.int32, (tile, 2 * LANES), 0).astype(jnp.float32).astype(jnp.bfloat16)

    def body(unused, state):
        out = []
        for s in range(2):
            first, last = state[2 * s], state[2 * s + 1]
            key = key_ref[s]
            next_first = jnp.min(jnp.where(key > first, key, BIG), axis=0, keepdims=True)
            next_last = jnp.max(jnp.where(key < last, key, -1.0), axis=0, keepdims=True)
            first_ok = next_first < last
            last_ok = next_last > next_first
            out += [next_first, next_last]
            heads, weights, locals_ = [], [], []
            for at, ok in ((next_first, first_ok), (next_last, last_ok)):
                start = jnp.where(ok, at, 0.0).astype(jnp.int32)
                window = take_windows(code_ref, length, start)
                item, session = window & item_mask, window >> ITEM_BITS
                linked = (session == session[16:17]) & near & ok
                heads.append(jnp.where(linked & (item < rows), item, -1).astype(jnp.float32))
                weights.append(jnp.sum(jnp.where(linked, 1.0, 0.0), axis=0, keepdims=True))
                locals_.append(item[16:17] - base - s * band)
            head = jnp.concatenate(heads, axis=1)
            weight = jnp.concatenate(weights, axis=1)
            local = jnp.concatenate(locals_, axis=1)
            links = jnp.zeros((rows, 2 * LANES), jnp.bfloat16)
            for d in range(1, 32):
                if d != 16:
                    links += hot_columns(row_ids, head[d : d + 1])
            upper = local >= half
            side = jnp.broadcast_to(jnp.where(upper, 1.0, 0.0), (16, 2 * LANES)).astype(jnp.bfloat16)
            high_part = jnp.concatenate([links[n : n + 16] * side for n in range(0, rows, 16)], axis=0)
            pair = jnp.concatenate([links - high_part, high_part], axis=0)
            inner = jnp.where(upper, local - half, local)
            for t in range(half // tile):
                inside = (inner >= t * tile) & (inner < (t + 1) * tile)
                hot = hot_columns(t_ids, jnp.where(inside, inner - t * tile, -1).astype(jnp.float32))
                count_ref[s, :, t * tile : (t + 1) * tile] += lax.dot_general(
                    pair, hot, NT, preferred_element_type=jnp.float32
                )
            coarse = jnp.where(m_ids == (local >> 7), weight, 0.0).astype(jnp.bfloat16)
            fine = one_where(l_ids == (local & (LANES - 1)))
            margin_ref[s] += lax.dot_general(coarse, fine, NT, preferred_element_type=jnp.float32)
        return tuple(out)

    low = jnp.full((1, LANES), -1.0, jnp.float32)
    high = jnp.full((1, LANES), BIG, jnp.float32)
    lax.fori_loop(0, trips, body, (low, high, low, high))


def sketch_kernel(
    slabs, rows, half, width, scale, count_ref, margin_ref, head_ref, bits_ref, out_ref,
    log_ref, own_bits, head_bits, acc_ref, send_ref, recv_ref, bit_sems, send_sems, recv_sems,
):
    me = lax.axis_index("stream")
    barrier = greet_all(slabs, me)
    owned = 4 * half
    share = rows // slabs
    tile = min(half, 512)
    bit_copy = pltpu.make_async_copy(
        bits_ref.at[:, pl.ds(pl.multiple_of(me * owned, owned), owned)], own_bits, bit_sems.at[0]
    )
    head_copy = pltpu.make_async_copy(bits_ref.at[:, 0:rows], head_bits, bit_sems.at[1])
    bit_copy.start()
    head_copy.start()

    log_ref[...] = jnp.log(jnp.maximum(margin_ref[...], 1.0))
    row_log = jnp.log(jnp.maximum(head_ref[share : share + 1], 1.0))
    column_log = jnp.broadcast_to(row_log, (rows, LANES)).T
    total_log = jnp.log(jnp.sum(head_ref[share + 1 : share + 2], axis=1, keepdims=True))
    row_term = total_log - column_log[:, 0:1]
    groups = []
    for g in range(width // 8):
        word = 8 * g // BITS_PER_WORD
        groups.append((word, (word + 1) * BITS_PER_WORD - 8 * g, 8 * g - word * BITS_PER_WORD))

    def product(positive, words):
        size = words.shape[1]
        shift = lax.broadcasted_iota(jnp.int32, (8, size), 0)
        upper = positive.astype(jnp.bfloat16)
        lower = (positive - upper.astype(jnp.float32)).astype(jnp.bfloat16)
        parts = []
        for word, split, offset in groups:
            now = jnp.broadcast_to(words[word : word + 1], (8, size))
            where_bit = shift + offset
            if split < 8:
                later = jnp.broadcast_to(words[word + 1 : word + 2], (8, size))
                now = jnp.where(shift >= split, later, now)
                where_bit = jnp.where(shift >= split, shift - split, where_bit)
            parts.append(jnp.where(((now >> where_bit) & 1) == 1, 1.0, -1.0))
        signs = jnp.concatenate(parts, axis=0).astype(jnp.bfloat16)
        both = jnp.concatenate([upper, lower], axis=0)
        value = lax.dot_general(both, signs, NT, preferred_element_type=jnp.float32)
        return value[0:rows] + value[rows:]

    head_copy.wait()
    row = lax.broadcasted_iota(jnp.int32, (8, LANES), 0)
    shared = jnp.concatenate(
        [jnp.where(row < share, head_ref[...], 0.0), jnp.zeros((rows - 8, LANES), jnp.float32)], axis=0
    )
    shared = pltpu.roll(shared, me * share, 0)
    ratio = jnp.log(jnp.maximum(shared, 1.0)) + total_log - row_log - column_log
    first_band = jnp.where(lax.axis_index("item") == 0, 1.0, 0.0)
    positive = jnp.where(shared > 0, jnp.maximum(ratio, 0.0), 0.0) * first_band
    acc_ref[...] = product(positive.T, head_bits[...])
    bit_copy.wait()

    for s in range(2):
        for h in range(2):

            def step(t, unused, s=s, h=h):
                at = pl.multiple_of(t * tile, tile)
                counts = count_ref[s, h * rows : (h + 1) * rows, pl.ds(at, tile)]
                first_log = h * (half // LANES) + t * (tile // LANES)
                col_log = jnp.concatenate(
                    [log_ref[s, pl.ds(first_log + n, 1), :] for n in range(tile // LANES)], axis=1
                )
                ratio = jnp.log(jnp.maximum(counts, 1.0)) + row_term - col_log
                positive = jnp.where(counts > 0, jnp.maximum(ratio, 0.0), 0.0)
                bit_at = pl.multiple_of(s * 2 * half + h * half + t * tile, tile)
                acc_ref[...] += product(positive, own_bits[:, pl.ds(bit_at, tile)])
                return unused

            lax.fori_loop(0, half // tile, step, 0)

    cuts = width // LANES
    for d in range(slabs):
        for c in range(cuts):
            send_ref[d, c * share : (c + 1) * share] = (
                acc_ref[d * share : (d + 1) * share, c * LANES : (c + 1) * LANES] * scale
            )
    pl.semaphore_wait(barrier, slabs - 1)
    exchange(slabs, me, send_ref, recv_ref, send_sems, recv_sems, True)
    exchange(slabs, me, send_ref, recv_ref, send_sems, recv_sems, False)
    summed = jnp.sum(recv_ref[...], axis=0)
    out_ref[...] = jnp.concatenate([summed[c * share : (c + 1) * share] for c in range(cuts)], axis=1)


def local(event_items, event_sessions, sketch_bits):
    slabs = lax.axis_size("stream")
    slab = event_items.shape[0]
    total_events = slab * slabs
    words, band_size = sketch_bits.shape
    owned = band_size // slabs
    rows, width, half = 128, 256, owned // 4
    me = lax.axis_index("stream")
    own_start = me * owned
    first_id = lax.axis_index("item") * band_size + own_start
    blocks = slab // LANES
    length = total_events // LANES

    dma = pltpu.SemaphoreType.DMA
    all_items, all_sessions, head = pl.pallas_call(
        functools.partial(gather_kernel, slabs, rows, blocks),
        out_shape=(
            jax.ShapeDtypeStruct((slabs, blocks, LANES), jnp.int32),
            jax.ShapeDtypeStruct((slabs, blocks, LANES), jnp.int16),
            jax.ShapeDtypeStruct((8, LANES), jnp.float32),
        ),
        in_specs=[VMEM, VMEM],
        out_specs=(VMEM, VMEM, VMEM),
        scratch_shapes=[
            pltpu.VMEM((blocks, LANES), jnp.int16),
            pltpu.VMEM((4, 8, LANES), jnp.int32),
            pltpu.VMEM((blocks + 16, LANES), jnp.int32),
            pltpu.VMEM((blocks + 16, LANES), jnp.int32),
            pltpu.VMEM((rows + 8, LANES), jnp.float32),
            pltpu.VMEM((8, LANES), jnp.float32),
            pltpu.VMEM((slabs, 8, LANES), jnp.float32),
            pltpu.VMEM((slabs, 8, LANES), jnp.float32),
            dma((slabs,)),
            dma((slabs,)),
            dma((slabs,)),
            dma((slabs,)),
            dma((4,)),
            dma((4,)),
            dma((slabs,)),
            dma((slabs,)),
        ],
        compiler_params=pltpu.CompilerParams(
            collective_id=0, has_side_effects=True, vmem_limit_bytes=VMEM_GRANT
        ),
        name="gather_events",
    )(event_items.reshape(blocks, LANES), event_sessions.reshape(blocks, LANES))

    band_rows = max(8, 2 * half // LANES)
    counts, margins = pl.pallas_call(
        functools.partial(tile_kernel, rows, length, half),
        out_shape=(
            jax.ShapeDtypeStruct((2, 2 * rows, half), jnp.float32),
            jax.ShapeDtypeStruct((2, band_rows, LANES), jnp.float32),
        ),
        in_specs=[pl.BlockSpec(memory_space=pltpu.SMEM), VMEM, VMEM],
        out_specs=(VMEM, VMEM),
        scratch_shapes=[
            pltpu.VMEM((length, LANES), jnp.int32),
            pltpu.VMEM((length + 32, LANES), jnp.int32),
            pltpu.VMEM((2, length, LANES), jnp.float32),
        ],
        compiler_params=pltpu.CompilerParams(vmem_limit_bytes=VMEM_GRANT),
        name="tile_counts",
    )(first_id.astype(jnp.int32)[None], all_items, all_sessions)

    own_rows = pl.pallas_call(
        functools.partial(sketch_kernel, slabs, rows, half, width, 1.0 / math.sqrt(total_events)),
        out_shape=jax.ShapeDtypeStruct((rows // slabs, width), jnp.float32),
        in_specs=[VMEM] * 3 + [pl.BlockSpec(memory_space=pl.ANY)],
        out_specs=VMEM,
        scratch_shapes=[
            pltpu.VMEM((2, band_rows, LANES), jnp.float32),
            pltpu.VMEM((words, owned), jnp.int32),
            pltpu.VMEM((words, rows), jnp.int32),
            pltpu.VMEM((rows, width), jnp.float32),
            pltpu.VMEM((slabs, 8, LANES), jnp.float32),
            pltpu.VMEM((slabs, 8, LANES), jnp.float32),
            dma((2,)),
            dma((slabs,)),
            dma((slabs,)),
        ],
        compiler_params=pltpu.CompilerParams(
            collective_id=1, has_side_effects=True, vmem_limit_bytes=VMEM_GRANT
        ),
        name="sketch_tile",
    )(counts, margins, head, sketch_bits)
    if lax.axis_size("item") > 1:
        own_rows = lax.psum(own_rows, "item")
    return own_rows


def solution(mesh):
    placed = (P("stream"), P("stream"), P(None, "item"))
    return jax.shard_map(
        local, mesh=mesh, in_specs=placed, out_specs=P("stream", None), check_vma=False
    )
```

```python
import functools
import math

import jax
import jax.numpy as jnp
from jax import lax
from jax.experimental import pallas as pl
from jax.experimental.pallas import tpu as pltpu
from jax.sharding import PartitionSpec as P

WINDOW = 15
ITEM_BITS = 18
LANES = 128
BITS_PER_WORD = 18
BIG = 1.0e6
VMEM_GRANT = 45 * 1024 * 1024
NT = (((1,), (1,)), ((), ()))
VMEM = pl.BlockSpec(memory_space=pltpu.VMEM)


def one_where(mask):
    return jnp.where(mask, 1.0, 0.0).astype(jnp.bfloat16)


def hot_columns(ids, values):
    row = jnp.broadcast_to(values, (16, values.shape[1])).astype(jnp.bfloat16)
    one, zero = jnp.ones((), jnp.bfloat16), jnp.zeros((), jnp.bfloat16)
    return jnp.concatenate(
        [jnp.where(ids[n : n + 16] == row, one, zero) for n in range(0, ids.shape[0], 16)], axis=0
    )


def greet_all(slabs, me):
    barrier = pltpu.get_barrier_semaphore()

    for k in range(1, slabs):
        pl.semaphore_signal(
            barrier, inc=1, device_id={"stream": lax.rem(me + k, slabs)}, device_id_type=pl.DeviceIdType.MESH
        )
    return barrier


def send(src, dst, send_sem, recv_sem, to):
    return pltpu.make_async_remote_copy(
        src_ref=src,
        dst_ref=dst,
        send_sem=send_sem,
        recv_sem=recv_sem,
        device_id={"stream": to},
        device_id_type=pl.DeviceIdType.MESH,
    )


def each(low, high, do):
    for k in range(low, high):
        do(k)


def exchange(slabs, me, out_ref, in_ref, send_sems, recv_sems, start):
    def copy(k):
        to = lax.rem(me + k, slabs)
        return send(out_ref.at[to], in_ref.at[me], send_sems.at[k], recv_sems.at[k], to)

    if start:
        each(1, slabs, lambda k: copy(k).start())
        in_ref[me] = out_ref[me]
    else:
        each(1, slabs, lambda k: copy(k).wait())


def gather_kernel(
    slabs, rows, blocks, own_ref, all_items, all_sessions, head_ref,
    short_ref, halo_ref, item_ref, session_ref, links_ref, total_ref,
    head_out, head_in, far_send, far_recv, near_send, near_recv, halo_send, halo_recv, head_send, head_recv,
):
    me = lax.axis_index("stream")
    partner = me + 1 - 2 * lax.rem(me, 2)
    after, before = lax.rem(me + 1, slabs), lax.rem(me + slabs - 1, slabs)
    own_items, own_sessions = own_ref.at[0], own_ref.at[1]
    barrier = greet_all(slabs, me)
    short_ref[...] = own_sessions[...].astype(jnp.int16)
    item_ref[8 : 8 + blocks] = own_items[...]
    session_ref[8 : 8 + blocks] = own_sessions[...]
    all_items[me] = own_items[...]
    all_sessions[me] = short_ref[...]
    pl.semaphore_wait(barrier, slabs - 1)

    halos = []
    for n, ref in enumerate((own_items, own_sessions)):
        for side, to, rows_sent in ((0, after, ref.at[blocks - 8 : blocks]), (1, before, ref.at[0:8])):
            at = 2 * n + side
            halos.append(send(rows_sent, halo_ref.at[at], halo_send.at[at], halo_recv.at[at], to))
    for copy in halos:
        copy.start()

    pairs = ((own_items, all_items, 0), (short_ref, all_sessions, slabs // 2))

    def far(k):
        to = lax.rem(me + 2 * k, slabs)
        return [
            send(own, every.at[me], far_send.at[at + k], far_recv.at[at + k], to) for own, every, at in pairs
        ]

    def near(k):
        source = lax.rem(me + 2 * slabs - 2 * k, slabs)
        return [
            send(every.at[source], every.at[source], near_send.at[at + k], near_recv.at[at + k], partner)
            for own, every, at in pairs
        ]

    def do_all(copies, act):
        for copy in copies:
            act(copy)

    own_near = [
        send(own, every.at[me], near_send.at[at], near_recv.at[at], partner) for own, every, at in pairs
    ]
    each(1, slabs // 2, lambda k: do_all(far(k), lambda c: c.start()))
    do_all(own_near, lambda c: c.start())

    sub = lax.broadcasted_iota(jnp.int32, (LANES, LANES), 0)
    lane = lax.broadcasted_iota(jnp.int32, (LANES, LANES), 1)
    low_lane = lax.broadcasted_iota(jnp.int32, (1, LANES), 1) < LANES // 2
    ids = lax.broadcasted_iota(jnp.int32, (rows, LANES), 0)
    gaps = (sub - LANES // 2 - lane, sub + LANES // 2 - lane)
    in_reach = [(jnp.abs(gap) <= WINDOW) & (gap != 0) for gap in gaps]
    ones = jnp.ones((8, 2 * LANES), jnp.float32).astype(jnp.bfloat16)
    links_ref[...] = jnp.zeros_like(links_ref)
    total_ref[...] = jnp.zeros_like(total_ref)

    def block(b, unused):
        def around(ref):
            turned = [pltpu.roll(ref[pl.ds(b + o, 1)], LANES // 2, 1) for o in (7, 8, 9)]
            return (
                jnp.where(low_lane, turned[0], turned[1]),
                jnp.where(low_lane, turned[1], turned[2]),
            )

        own_item, own_session = item_ref[pl.ds(b + 8, 1)], session_ref[pl.ds(b + 8, 1)]
        hot = jnp.concatenate([one_where(ids == item) for item in around(item_ref)], axis=1)
        linked = jnp.concatenate(
            [
                one_where((jnp.broadcast_to(session, (LANES, LANES)).T == own_session) & reach)
                for session, reach in zip(around(session_ref), in_reach)
            ],
            axis=0,
        )
        links = jnp.dot(jnp.concatenate([hot, ones], axis=0), linked, preferred_element_type=jnp.float32)
        links_ref[...] += lax.dot_general(
            links.astype(jnp.bfloat16), one_where(ids == own_item), NT, preferred_element_type=jnp.float32
        )
        total_ref[...] += links[rows:]
        return unused

    lax.fori_loop(1, blocks - 1, block, 0, unroll=5)
    for copy in halos:
        copy.wait()
    item_ref[0:8] = halo_ref[0]
    item_ref[8 + blocks : 16 + blocks] = halo_ref[1]
    session_ref[0:8] = jnp.where(me == 0, -1, halo_ref[2])
    session_ref[8 + blocks : 16 + blocks] = jnp.where(me == slabs - 1, -1, halo_ref[3])
    block(0, 0)
    block(blocks - 1, 0)

    share = rows // slabs
    tail = jnp.concatenate([links_ref[rows : rows + 1], total_ref[0:1]], axis=0)
    for d in range(slabs):
        head_out[d, 0:share] = links_ref[d * share : (d + 1) * share]
        head_out[d, share : share + 2] = tail
        head_out[d, share + 2 : 8] = jnp.zeros((6 - share, LANES), jnp.float32)

    exchange(slabs, me, head_out, head_in, head_send, head_recv, True)

    def forward(k):
        do_all(far(k), lambda c: c.wait_recv())
        do_all(near(k), lambda c: c.start())

    each(1, slabs // 2, forward)
    exchange(slabs, me, head_out, head_in, head_send, head_recv, False)
    head_ref[...] = jnp.sum(head_in[...], axis=0)
    do_all(own_near, lambda c: c.wait())
    each(1, slabs // 2, lambda k: do_all(near(k), lambda c: c.wait()))
    each(1, slabs // 2, lambda k: do_all(far(k), lambda c: c.wait_send()))


def take_windows(code_ref, length, start):
    whole, part = start >> 3, start & 7
    bits = max(1, (length // 8 - 1).bit_length())
    keep = 8 * ((1 << (bits - 1)) + 4)
    value = None
    for bit in reversed(range(bits)):
        step = 8 << bit
        keep = 8 * ((1 << bit) + 4)
        chosen = ((whole >> bit) & 1) == 1
        if value is None:
            low, high = code_ref[0:keep, :], code_ref[step : step + keep, :]
        else:
            low, high = value[0:keep], value[step : step + keep]
        value = jnp.where(chosen, high, low)
    for bit in (2, 1, 0):
        chosen = ((part >> bit) & 1) == 1
        value = jnp.where(chosen, pltpu.roll(value, value.shape[0] - (1 << bit), 0), value)
    return value[0:32]


def tile_kernel(rows, length, half, base_ref, all_items, all_sessions, count_ref, margin_ref, flat_ref, code_ref, key_ref):
    item_mask = (1 << ITEM_BITS) - 1
    base = base_ref[0]
    count_ref[...] = jnp.zeros_like(count_ref)
    margin_ref[...] = jnp.zeros_like(margin_ref)
    band = 2 * half
    band_rows = band // LANES
    chunk = 8 * math.gcd(length // 8, 16)
    slabs, blocks, unused_lanes = all_items.shape
    for n in range(slabs):
        flat_ref[n * blocks : (n + 1) * blocks] = all_items[n] | (all_sessions[n].astype(jnp.int32) << ITEM_BITS)
    per = length // LANES
    for r in range(per):
        code_ref[16 + r * LANES : 16 + (r + 1) * LANES] = flat_ref[pl.ds(r, LANES, stride=per), :].T
    lane = lax.broadcasted_iota(jnp.int32, (16, LANES), 1)
    code_ref[0:16] = jnp.where(lane == 0, -1, pltpu.roll(code_ref[length : length + 16], 1, 1))
    code_ref[length + 16 : length + 32] = jnp.where(
        lane == LANES - 1, -1, pltpu.roll(code_ref[16:32], LANES - 1, 1)
    )

    def fill(c, tops):
        at = pl.multiple_of(c * chunk, chunk)
        item = code_ref[pl.ds(at + 16, chunk), :] & item_mask
        place = (at + lax.broadcasted_iota(jnp.int32, (chunk, LANES), 0)).astype(jnp.float32)
        new = []
        for s in range(2):
            local = item - base - s * band
            mine = (local >= 0) & (local < band) & (item >= rows)
            key_ref[s, pl.ds(at, chunk), :] = jnp.where(mine, place, BIG)
            new.append(tops[s] + jnp.sum(mine.astype(jnp.int32), axis=0, keepdims=True))
        return tuple(new)

    none = jnp.zeros((1, LANES), jnp.int32)
    tally = lax.fori_loop(0, length // chunk, fill, (none, none))
    trips = (jnp.max(jnp.maximum(tally[0], tally[1])) + 1) // 2

    row_ids = lax.broadcasted_iota(jnp.int32, (rows, 2 * LANES), 0).astype(jnp.float32).astype(jnp.bfloat16)
    d_ids = lax.broadcasted_iota(jnp.int32, (32, LANES), 0)
    near = (d_ids >= 1) & (d_ids != 16)
    m_ids = lax.broadcasted_iota(jnp.int32, (max(8, band_rows), 2 * LANES), 0)
    l_ids = lax.broadcasted_iota(jnp.int32, (LANES, 2 * LANES), 0)
    tile = 256
    t_ids = lax.broadcasted_iota(jnp.int32, (tile, 2 * LANES), 0).astype(jnp.float32).astype(jnp.bfloat16)

    def body(unused, state):
        out = []
        for s in range(2):
            first, last = state[2 * s], state[2 * s + 1]
            key = key_ref[s]
            next_first = jnp.min(jnp.where(key > first, key, BIG), axis=0, keepdims=True)
            next_last = jnp.max(jnp.where(key < last, key, -1.0), axis=0, keepdims=True)
            first_ok = next_first < last
            last_ok = next_last > next_first
            out += [next_first, next_last]
            heads, weights, locals_ = [], [], []
            for at, ok in ((next_first, first_ok), (next_last, last_ok)):
                start = jnp.where(ok, at, 0.0).astype(jnp.int32)
                window = take_windows(code_ref, length, start)
                item, session = window & item_mask, window >> ITEM_BITS
                linked = (session == session[16:17]) & near & ok
                heads.append(jnp.where(linked & (item < rows), item, -1).astype(jnp.float32))
                weights.append(jnp.sum(jnp.where(linked, 1.0, 0.0), axis=0, keepdims=True))
                locals_.append(item[16:17] - base - s * band)
            head = jnp.concatenate(heads, axis=1)
            weight = jnp.concatenate(weights, axis=1)
            local = jnp.concatenate(locals_, axis=1)
            links = jnp.zeros((rows, 2 * LANES), jnp.bfloat16)
            for d in range(1, 32):
                if d != 16:
                    links += hot_columns(row_ids, head[d : d + 1])
            upper = local >= half
            side = jnp.broadcast_to(jnp.where(upper, 1.0, 0.0), (16, 2 * LANES)).astype(jnp.bfloat16)
            high_part = jnp.concatenate([links[n : n + 16] * side for n in range(0, rows, 16)], axis=0)
            pair = jnp.concatenate([links - high_part, high_part], axis=0)
            inner = jnp.where(upper, local - half, local)
            for t in range(half // tile):
                inside = (inner >= t * tile) & (inner < (t + 1) * tile)
                hot = hot_columns(t_ids, jnp.where(inside, inner - t * tile, -1).astype(jnp.float32))
                count_ref[s, :, t * tile : (t + 1) * tile] += lax.dot_general(
                    pair, hot, NT, preferred_element_type=jnp.float32
                )
            coarse = jnp.where(m_ids == (local >> 7), weight, 0.0).astype(jnp.bfloat16)
            fine = one_where(l_ids == (local & (LANES - 1)))
            margin_ref[s] += lax.dot_general(coarse, fine, NT, preferred_element_type=jnp.float32)
        return tuple(out)

    low = jnp.full((1, LANES), -1.0, jnp.float32)
    high = jnp.full((1, LANES), BIG, jnp.float32)
    lax.fori_loop(0, trips, body, (low, high, low, high))


def sketch_kernel(
    slabs, rows, half, width, scale, count_ref, margin_ref, head_ref, bits_ref, out_ref,
    log_ref, own_bits, head_bits, acc_ref, send_ref, recv_ref, bit_sems, send_sems, recv_sems,
):
    me = lax.axis_index("stream")
    barrier = greet_all(slabs, me)
    owned = 4 * half
    share = rows // slabs
    tile = min(half, 512)
    bit_copy = pltpu.make_async_copy(
        bits_ref.at[:, pl.ds(pl.multiple_of(me * owned, owned), owned)], own_bits, bit_sems.at[0]
    )
    head_copy = pltpu.make_async_copy(bits_ref.at[:, 0:rows], head_bits, bit_sems.at[1])
    bit_copy.start()
    head_copy.start()

    log_ref[...] = jnp.log(jnp.maximum(margin_ref[...], 1.0))
    row_log = jnp.log(jnp.maximum(head_ref[share : share + 1], 1.0))
    column_log = jnp.broadcast_to(row_log, (rows, LANES)).T
    total_log = jnp.log(jnp.sum(head_ref[share + 1 : share + 2], axis=1, keepdims=True))
    row_term = total_log - column_log[:, 0:1]
    groups = []
    for g in range(width // 8):
        word = 8 * g // BITS_PER_WORD
        groups.append((word, (word + 1) * BITS_PER_WORD - 8 * g, 8 * g - word * BITS_PER_WORD))

    def product(positive, words):
        size = words.shape[1]

        def wide(value):
            return jnp.concatenate([value] * (size // LANES), axis=1)

        shift = lax.broadcasted_iota(jnp.int32, (8, LANES), 0)
        upper = positive.astype(jnp.bfloat16)
        lower = (positive - upper.astype(jnp.float32)).astype(jnp.bfloat16)
        parts = []
        for word, split, offset in groups:
            now = jnp.broadcast_to(words[word : word + 1], (8, size))
            where_bit = jnp.left_shift(1, shift + offset)
            if split < 8:
                later = jnp.broadcast_to(words[word + 1 : word + 2], (8, size))
                now = jnp.where(wide(shift) >= split, later, now)
                place = jnp.where(shift >= split, shift - split, shift + offset)
                where_bit = jnp.left_shift(1, place)
            parts.append(jnp.where((now & wide(where_bit)) != 0, 1.0, -1.0))
        signs = jnp.concatenate(parts, axis=0).astype(jnp.bfloat16)
        both = jnp.concatenate([upper, lower], axis=0)
        value = lax.dot_general(both, signs, NT, preferred_element_type=jnp.float32)
        return value[0:rows] + value[rows:]

    head_copy.wait()
    row = lax.broadcasted_iota(jnp.int32, (8, LANES), 0)
    shared = jnp.concatenate(
        [jnp.where(row < share, head_ref[...], 0.0), jnp.zeros((rows - 8, LANES), jnp.float32)], axis=0
    )
    shared = pltpu.roll(shared, me * share, 0)
    ratio = jnp.log(jnp.maximum(shared, 1.0)) + total_log - row_log - column_log
    first_band = jnp.where(lax.axis_index("item") == 0, 1.0, 0.0)
    positive = jnp.where(shared > 0, jnp.maximum(ratio, 0.0), 0.0) * first_band
    acc_ref[...] = product(positive.T, head_bits[...])
    bit_copy.wait()

    for s in range(2):
        for h in range(2):

            def step(t, unused, s=s, h=h):
                at = pl.multiple_of(t * tile, tile)
                counts = count_ref[s, h * rows : (h + 1) * rows, pl.ds(at, tile)]
                first_log = h * (half // LANES) + t * (tile // LANES)
                col_log = jnp.concatenate(
                    [log_ref[s, pl.ds(first_log + n, 1), :] for n in range(tile // LANES)], axis=1
                )
                ratio = jnp.log(jnp.maximum(counts, 1.0)) + row_term - col_log
                positive = jnp.where(counts > 0, jnp.maximum(ratio, 0.0), 0.0)
                bit_at = pl.multiple_of(s * 2 * half + h * half + t * tile, tile)
                acc_ref[...] += product(positive, own_bits[:, pl.ds(bit_at, tile)])
                return unused

            lax.fori_loop(0, half // tile, step, 0)

    cuts = width // LANES
    for d in range(slabs):
        for c in range(cuts):
            send_ref[d, c * share : (c + 1) * share] = (
                acc_ref[d * share : (d + 1) * share, c * LANES : (c + 1) * LANES] * scale
            )
    pl.semaphore_wait(barrier, slabs - 1)
    exchange(slabs, me, send_ref, recv_ref, send_sems, recv_sems, True)
    exchange(slabs, me, send_ref, recv_ref, send_sems, recv_sems, False)
    summed = jnp.sum(recv_ref[...], axis=0)
    out_ref[...] = jnp.concatenate([summed[c * share : (c + 1) * share] for c in range(cuts)], axis=1)


def local(event_items, event_sessions, sketch_bits):
    slabs = lax.axis_size("stream")
    slab = event_items.shape[0]
    total_events = slab * slabs
    words, band_size = sketch_bits.shape
    owned = band_size // slabs
    rows, width, half = 128, 256, owned // 4
    me = lax.axis_index("stream")
    own_start = me * owned
    first_id = lax.axis_index("item") * band_size + own_start
    blocks = slab // LANES
    length = total_events // LANES

    dma = pltpu.SemaphoreType.DMA
    all_items, all_sessions, head = pl.pallas_call(
        functools.partial(gather_kernel, slabs, rows, blocks),
        out_shape=(
            jax.ShapeDtypeStruct((slabs, blocks, LANES), jnp.int32),
            jax.ShapeDtypeStruct((slabs, blocks, LANES), jnp.int16),
            jax.ShapeDtypeStruct((8, LANES), jnp.float32),
        ),
        in_specs=[VMEM],
        out_specs=(VMEM, VMEM, VMEM),
        scratch_shapes=[
            pltpu.VMEM((blocks, LANES), jnp.int16),
            pltpu.VMEM((4, 8, LANES), jnp.int32),
            pltpu.VMEM((blocks + 16, LANES), jnp.int32),
            pltpu.VMEM((blocks + 16, LANES), jnp.int32),
            pltpu.VMEM((rows + 8, LANES), jnp.float32),
            pltpu.VMEM((8, LANES), jnp.float32),
            pltpu.VMEM((slabs, 8, LANES), jnp.float32),
            pltpu.VMEM((slabs, 8, LANES), jnp.float32),
            dma((slabs,)),
            dma((slabs,)),
            dma((slabs,)),
            dma((slabs,)),
            dma((4,)),
            dma((4,)),
            dma((slabs,)),
            dma((slabs,)),
        ],
        compiler_params=pltpu.CompilerParams(
            collective_id=0, has_side_effects=True, vmem_limit_bytes=VMEM_GRANT
        ),
        name="gather_events",
    )(jnp.stack([event_items, event_sessions]).reshape(2, blocks, LANES))

    band_rows = max(8, 2 * half // LANES)
    counts, margins = pl.pallas_call(
        functools.partial(tile_kernel, rows, length, half),
        out_shape=(
            jax.ShapeDtypeStruct((2, 2 * rows, half), jnp.float32),
            jax.ShapeDtypeStruct((2, band_rows, LANES), jnp.float32),
        ),
        in_specs=[pl.BlockSpec(memory_space=pltpu.SMEM), VMEM, VMEM],
        out_specs=(VMEM, VMEM),
        scratch_shapes=[
            pltpu.VMEM((length, LANES), jnp.int32),
            pltpu.VMEM((length + 32, LANES), jnp.int32),
            pltpu.VMEM((2, length, LANES), jnp.float32),
        ],
        compiler_params=pltpu.CompilerParams(vmem_limit_bytes=VMEM_GRANT),
        name="tile_counts",
    )(first_id.astype(jnp.int32)[None], all_items, all_sessions)

    own_rows = pl.pallas_call(
        functools.partial(sketch_kernel, slabs, rows, half, width, 1.0 / math.sqrt(total_events)),
        out_shape=jax.ShapeDtypeStruct((rows // slabs, width), jnp.float32),
        in_specs=[VMEM] * 3 + [pl.BlockSpec(memory_space=pl.ANY)],
        out_specs=VMEM,
        scratch_shapes=[
            pltpu.VMEM((2, band_rows, LANES), jnp.float32),
            pltpu.VMEM((words, owned), jnp.int32),
            pltpu.VMEM((words, rows), jnp.int32),
            pltpu.VMEM((rows, width), jnp.float32),
            pltpu.VMEM((slabs, 8, LANES), jnp.float32),
            pltpu.VMEM((slabs, 8, LANES), jnp.float32),
            dma((2,)),
            dma((slabs,)),
            dma((slabs,)),
        ],
        compiler_params=pltpu.CompilerParams(
            collective_id=1, has_side_effects=True, vmem_limit_bytes=VMEM_GRANT
        ),
        name="sketch_tile",
    )(counts, margins, head, sketch_bits)
    if lax.axis_size("item") > 1:
        own_rows = lax.psum(own_rows, "item")
    return own_rows


def solution(mesh):
    placed = (P("stream"), P("stream"), P(None, "item"))
    return jax.shard_map(
        local, mesh=mesh, in_specs=placed, out_specs=P("stream", None), check_vma=False
    )
```

```python
import functools
import math

import jax
import jax.numpy as jnp
from jax import lax
from jax.experimental import pallas as pl
from jax.experimental.pallas import tpu as pltpu
from jax.sharding import PartitionSpec as P

WINDOW = 15
ITEM_BITS = 18
LANES = 128
BITS_PER_WORD = 18
BIG = 1.0e6
VMEM_GRANT = 45 * 1024 * 1024
NT = (((1,), (1,)), ((), ()))
VMEM = pl.BlockSpec(memory_space=pltpu.VMEM)


def one_where(mask):
    return jnp.where(mask, 1.0, 0.0).astype(jnp.bfloat16)


def hot_columns(ids, values):
    row = jnp.broadcast_to(values, (16, values.shape[1])).astype(jnp.bfloat16)
    one, zero = jnp.ones((), jnp.bfloat16), jnp.zeros((), jnp.bfloat16)
    return jnp.concatenate(
        [jnp.where(ids[n : n + 16] == row, one, zero) for n in range(0, ids.shape[0], 16)], axis=0
    )


def greet_all(slabs, me):
    barrier = pltpu.get_barrier_semaphore()

    for k in range(1, slabs):
        pl.semaphore_signal(
            barrier, inc=1, device_id={"stream": lax.rem(me + k, slabs)}, device_id_type=pl.DeviceIdType.MESH
        )
    return barrier


def send(src, dst, send_sem, recv_sem, to):
    return pltpu.make_async_remote_copy(
        src_ref=src,
        dst_ref=dst,
        send_sem=send_sem,
        recv_sem=recv_sem,
        device_id={"stream": to},
        device_id_type=pl.DeviceIdType.MESH,
    )


def each(low, high, do):
    for k in range(low, high):
        do(k)


def exchange(slabs, me, out_ref, in_ref, send_sems, recv_sems, start):
    def copy(k):
        to = lax.rem(me + k, slabs)
        return send(out_ref.at[to], in_ref.at[me], send_sems.at[k], recv_sems.at[k], to)

    if start:
        each(1, slabs, lambda k: copy(k).start())
        in_ref[me] = out_ref[me]
    else:
        each(1, slabs, lambda k: copy(k).wait())


def gather_kernel(
    slabs, rows, blocks, own_ref, all_items, all_sessions, head_ref,
    short_ref, halo_ref, item_ref, session_ref, links_ref, total_ref,
    head_out, head_in, far_send, far_recv, near_send, near_recv, halo_send, halo_recv, head_send, head_recv,
):
    me = lax.axis_index("stream")
    partner = me + 1 - 2 * lax.rem(me, 2)
    after, before = lax.rem(me + 1, slabs), lax.rem(me + slabs - 1, slabs)
    own_items, own_sessions = own_ref.at[0], own_ref.at[1]
    barrier = greet_all(slabs, me)
    short_ref[...] = own_sessions[...].astype(jnp.int16)
    item_ref[8 : 8 + blocks] = own_items[...]
    session_ref[8 : 8 + blocks] = own_sessions[...]
    all_items[me] = own_items[...]
    all_sessions[me] = short_ref[...]
    pl.semaphore_wait(barrier, slabs - 1)

    halos = []
    for n, ref in enumerate((own_items, own_sessions)):
        for side, to, rows_sent in ((0, after, ref.at[blocks - 8 : blocks]), (1, before, ref.at[0:8])):
            at = 2 * n + side
            halos.append(send(rows_sent, halo_ref.at[at], halo_send.at[at], halo_recv.at[at], to))
    for copy in halos:
        copy.start()

    pairs = ((own_items, all_items, 0), (short_ref, all_sessions, slabs // 2))

    def far(k):
        to = lax.rem(me + 2 * k, slabs)
        return [
            send(own, every.at[me], far_send.at[at + k], far_recv.at[at + k], to) for own, every, at in pairs
        ]

    def near(k):
        source = lax.rem(me + 2 * slabs - 2 * k, slabs)
        return [
            send(every.at[source], every.at[source], near_send.at[at + k], near_recv.at[at + k], partner)
            for own, every, at in pairs
        ]

    def do_all(copies, act):
        for copy in copies:
            act(copy)

    own_near = [
        send(own, every.at[me], near_send.at[at], near_recv.at[at], partner) for own, every, at in pairs
    ]
    each(1, slabs // 2, lambda k: do_all(far(k), lambda c: c.start()))
    do_all(own_near, lambda c: c.start())

    sub = lax.broadcasted_iota(jnp.int32, (LANES, LANES), 0)
    lane = lax.broadcasted_iota(jnp.int32, (LANES, LANES), 1)
    low_lane = lax.broadcasted_iota(jnp.int32, (1, LANES), 1) < LANES // 2
    ids = lax.broadcasted_iota(jnp.int32, (rows, LANES), 0)
    gaps = (sub - LANES // 2 - lane, sub + LANES // 2 - lane)
    in_reach = [(jnp.abs(gap) <= WINDOW) & (gap != 0) for gap in gaps]
    ones = jnp.ones((8, 2 * LANES), jnp.float32).astype(jnp.bfloat16)
    links_ref[...] = jnp.zeros_like(links_ref)
    total_ref[...] = jnp.zeros_like(total_ref)

    def block(b, unused):
        def around(ref):
            turned = [pltpu.roll(ref[pl.ds(b + o, 1)], LANES // 2, 1) for o in (7, 8, 9)]
            return (
                jnp.where(low_lane, turned[0], turned[1]),
                jnp.where(low_lane, turned[1], turned[2]),
            )

        own_item, own_session = item_ref[pl.ds(b + 8, 1)], session_ref[pl.ds(b + 8, 1)]
        hot = jnp.concatenate([one_where(ids == item) for item in around(item_ref)], axis=1)
        linked = jnp.concatenate(
            [
                one_where((jnp.broadcast_to(session, (LANES, LANES)).T == own_session) & reach)
                for session, reach in zip(around(session_ref), in_reach)
            ],
            axis=0,
        )
        links = jnp.dot(jnp.concatenate([hot, ones], axis=0), linked, preferred_element_type=jnp.float32)
        links_ref[...] += lax.dot_general(
            links.astype(jnp.bfloat16), one_where(ids == own_item), NT, preferred_element_type=jnp.float32
        )
        total_ref[...] += links[rows:]
        return unused

    lax.fori_loop(1, blocks - 1, block, 0, unroll=5)
    for copy in halos:
        copy.wait()
    item_ref[0:8] = halo_ref[0]
    item_ref[8 + blocks : 16 + blocks] = halo_ref[1]
    session_ref[0:8] = jnp.where(me == 0, -1, halo_ref[2])
    session_ref[8 + blocks : 16 + blocks] = jnp.where(me == slabs - 1, -1, halo_ref[3])
    block(0, 0)
    block(blocks - 1, 0)

    share = rows // slabs
    tail = jnp.concatenate([links_ref[rows : rows + 1], total_ref[0:1]], axis=0)
    for d in range(slabs):
        head_out[d, 0:share] = links_ref[d * share : (d + 1) * share]
        head_out[d, share : share + 2] = tail
        head_out[d, share + 2 : 8] = jnp.zeros((6 - share, LANES), jnp.float32)

    exchange(slabs, me, head_out, head_in, head_send, head_recv, True)

    def forward(k):
        do_all(far(k), lambda c: c.wait_recv())
        do_all(near(k), lambda c: c.start())

    each(1, slabs // 2, forward)
    exchange(slabs, me, head_out, head_in, head_send, head_recv, False)
    head_ref[...] = jnp.sum(head_in[...], axis=0)
    do_all(own_near, lambda c: c.wait())
    each(1, slabs // 2, lambda k: do_all(near(k), lambda c: c.wait()))
    each(1, slabs // 2, lambda k: do_all(far(k), lambda c: c.wait_send()))


def take_windows(code_ref, length, start):
    whole, part = start >> 3, start & 7
    bits = max(1, (length // 8 - 1).bit_length())
    keep = 8 * ((1 << (bits - 1)) + 4)
    value = None
    for bit in reversed(range(bits)):
        step = 8 << bit
        keep = 8 * ((1 << bit) + 4)
        chosen = ((whole >> bit) & 1) == 1
        if value is None:
            low, high = code_ref[0:keep, :], code_ref[step : step + keep, :]
        else:
            low, high = value[0:keep], value[step : step + keep]
        value = jnp.where(chosen, high, low)
    for bit in (2, 1, 0):
        chosen = ((part >> bit) & 1) == 1
        value = jnp.where(chosen, pltpu.roll(value, value.shape[0] - (1 << bit), 0), value)
    return value[0:32]


def tile_kernel(rows, length, half, base_ref, all_items, all_sessions, count_ref, margin_ref, flat_ref, code_ref, key_ref):
    item_mask = (1 << ITEM_BITS) - 1
    base = base_ref[0]
    count_ref[...] = jnp.zeros_like(count_ref)
    margin_ref[...] = jnp.zeros_like(margin_ref)
    band = 2 * half
    band_rows = band // LANES
    chunk = 8 * math.gcd(length // 8, 16)
    slabs, blocks, unused_lanes = all_items.shape
    for n in range(slabs):
        flat_ref[n * blocks : (n + 1) * blocks] = all_items[n] | (all_sessions[n].astype(jnp.int32) << ITEM_BITS)
    per = length // LANES
    for r in range(per):
        code_ref[16 + r * LANES : 16 + (r + 1) * LANES] = flat_ref[pl.ds(r, LANES, stride=per), :].T
    lane = lax.broadcasted_iota(jnp.int32, (16, LANES), 1)
    code_ref[0:16] = jnp.where(lane == 0, -1, pltpu.roll(code_ref[length : length + 16], 1, 1))
    code_ref[length + 16 : length + 32] = jnp.where(
        lane == LANES - 1, -1, pltpu.roll(code_ref[16:32], LANES - 1, 1)
    )

    def fill(c, tops):
        at = pl.multiple_of(c * chunk, chunk)
        item = code_ref[pl.ds(at + 16, chunk), :] & item_mask
        place = (at + lax.broadcasted_iota(jnp.int32, (chunk, LANES), 0)).astype(jnp.float32)
        new = []
        for s in range(2):
            local = item - base - s * band
            mine = (local >= 0) & (local < band) & (item >= rows)
            key_ref[s, pl.ds(at, chunk), :] = jnp.where(mine, place, BIG)
            new.append(tops[s] + jnp.sum(mine.astype(jnp.int32), axis=0, keepdims=True))
        return tuple(new)

    none = jnp.zeros((1, LANES), jnp.int32)
    tally = lax.fori_loop(0, length // chunk, fill, (none, none))
    trips = (jnp.max(jnp.maximum(tally[0], tally[1])) + 1) // 2

    row_ids = lax.broadcasted_iota(jnp.int32, (rows, 2 * LANES), 0).astype(jnp.float32).astype(jnp.bfloat16)
    d_ids = lax.broadcasted_iota(jnp.int32, (32, LANES), 0)
    near = (d_ids >= 1) & (d_ids != 16)
    m_ids = lax.broadcasted_iota(jnp.int32, (max(8, band_rows), 2 * LANES), 0)
    l_ids = lax.broadcasted_iota(jnp.int32, (LANES, 2 * LANES), 0)
    tile = 256
    t_ids = lax.broadcasted_iota(jnp.int32, (tile, 2 * LANES), 0).astype(jnp.float32).astype(jnp.bfloat16)

    def body(unused, state):
        out = []
        for s in range(2):
            first, last = state[2 * s], state[2 * s + 1]
            key = key_ref[s]
            next_first = jnp.min(jnp.where(key > first, key, BIG), axis=0, keepdims=True)
            next_last = jnp.max(jnp.where(key < last, key, -1.0), axis=0, keepdims=True)
            first_ok = next_first < last
            last_ok = next_last > next_first
            out += [next_first, next_last]
            heads, weights, locals_ = [], [], []
            for at, ok in ((next_first, first_ok), (next_last, last_ok)):
                start = jnp.where(ok, at, 0.0).astype(jnp.int32)
                window = take_windows(code_ref, length, start)
                item, session = window & item_mask, window >> ITEM_BITS
                linked = (session == session[16:17]) & near & ok
                heads.append(jnp.where(linked & (item < rows), item, -1).astype(jnp.float32))
                weights.append(jnp.sum(jnp.where(linked, 1.0, 0.0), axis=0, keepdims=True))
                locals_.append(item[16:17] - base - s * band)
            head = jnp.concatenate(heads, axis=1)
            weight = jnp.concatenate(weights, axis=1)
            local = jnp.concatenate(locals_, axis=1)
            links = jnp.zeros((rows, 2 * LANES), jnp.bfloat16)
            for d in range(1, 32):
                if d != 16:
                    links += hot_columns(row_ids, head[d : d + 1])
            upper = local >= half
            side = jnp.broadcast_to(jnp.where(upper, 1.0, 0.0), (16, 2 * LANES)).astype(jnp.bfloat16)
            high_part = jnp.concatenate([links[n : n + 16] * side for n in range(0, rows, 16)], axis=0)
            pair = jnp.concatenate([links - high_part, high_part], axis=0)
            inner = jnp.where(upper, local - half, local)
            for t in range(half // tile):
                inside = (inner >= t * tile) & (inner < (t + 1) * tile)
                hot = hot_columns(t_ids, jnp.where(inside, inner - t * tile, -1).astype(jnp.float32))
                count_ref[s, :, t * tile : (t + 1) * tile] += lax.dot_general(
                    pair, hot, NT, preferred_element_type=jnp.float32
                )
            coarse = jnp.where(m_ids == (local >> 7), weight, 0.0).astype(jnp.bfloat16)
            fine = one_where(l_ids == (local & (LANES - 1)))
            margin_ref[s] += lax.dot_general(coarse, fine, NT, preferred_element_type=jnp.float32)
        return tuple(out)

    low = jnp.full((1, LANES), -1.0, jnp.float32)
    high = jnp.full((1, LANES), BIG, jnp.float32)
    lax.fori_loop(0, trips, body, (low, high, low, high))


def sketch_kernel(
    slabs, rows, half, width, scale, count_ref, margin_ref, head_ref, bits_ref, out_ref,
    log_ref, own_bits, head_bits, acc_ref, send_ref, recv_ref, bit_sems, send_sems, recv_sems,
):
    me = lax.axis_index("stream")
    barrier = greet_all(slabs, me)
    owned = 4 * half
    share = rows // slabs
    tile = min(half, 512)
    bit_copy = pltpu.make_async_copy(
        bits_ref.at[:, pl.ds(pl.multiple_of(me * owned, owned), owned)], own_bits, bit_sems.at[0]
    )
    head_copy = pltpu.make_async_copy(bits_ref.at[:, 0:rows], head_bits, bit_sems.at[1])
    bit_copy.start()
    head_copy.start()

    log_ref[...] = jnp.log(jnp.maximum(margin_ref[...], 1.0))
    row_log = jnp.log(jnp.maximum(head_ref[share : share + 1], 1.0))
    column_log = jnp.broadcast_to(row_log, (rows, LANES)).T
    total_log = jnp.log(jnp.sum(head_ref[share + 1 : share + 2], axis=1, keepdims=True))
    row_term = total_log - column_log[:, 0:1]
    groups = []
    for g in range(width // 8):
        word = 8 * g // BITS_PER_WORD
        groups.append((word, (word + 1) * BITS_PER_WORD - 8 * g, 8 * g - word * BITS_PER_WORD))

    def product(positive, words):
        size = words.shape[1]

        def wide(value):
            return jnp.concatenate([value] * (size // LANES), axis=1)

        shift = lax.broadcasted_iota(jnp.int32, (8, LANES), 0)
        upper = positive.astype(jnp.bfloat16)
        lower = (positive - upper.astype(jnp.float32)).astype(jnp.bfloat16)
        parts = []
        for word, split, offset in groups:
            now = jnp.broadcast_to(words[word : word + 1], (8, size))
            where_bit = jnp.left_shift(1, shift + offset)
            if split < 8:
                later = jnp.broadcast_to(words[word + 1 : word + 2], (8, size))
                now = jnp.where(wide(shift) >= split, later, now)
                place = jnp.where(shift >= split, shift - split, shift + offset)
                where_bit = jnp.left_shift(1, place)
            parts.append(jnp.where((now & wide(where_bit)) != 0, 1.0, -1.0))
        signs = jnp.concatenate(parts, axis=0).astype(jnp.bfloat16)
        both = jnp.concatenate([upper, lower], axis=0)
        value = lax.dot_general(both, signs, NT, preferred_element_type=jnp.float32)
        return value[0:rows] + value[rows:]

    head_copy.wait()
    row = lax.broadcasted_iota(jnp.int32, (8, LANES), 0)
    shared = jnp.concatenate(
        [jnp.where(row < share, head_ref[...], 0.0), jnp.zeros((rows - 8, LANES), jnp.float32)], axis=0
    )
    shared = pltpu.roll(shared, me * share, 0)
    ratio = jnp.log(jnp.maximum(shared, 1.0)) + total_log - row_log - column_log
    first_band = jnp.where(lax.axis_index("item") == 0, 1.0, 0.0)
    positive = jnp.where(shared > 0, jnp.maximum(ratio, 0.0), 0.0) * first_band
    acc_ref[...] = product(positive.T, head_bits[...])
    bit_copy.wait()

    for s in range(2):
        for h in range(2):

            def step(t, unused, s=s, h=h):
                at = pl.multiple_of(t * tile, tile)
                counts = count_ref[s, h * rows : (h + 1) * rows, pl.ds(at, tile)]
                first_log = h * (half // LANES) + t * (tile // LANES)
                col_log = jnp.concatenate(
                    [log_ref[s, pl.ds(first_log + n, 1), :] for n in range(tile // LANES)], axis=1
                )
                ratio = jnp.log(jnp.maximum(counts, 1.0)) + row_term - col_log
                positive = jnp.where(counts > 0, jnp.maximum(ratio, 0.0), 0.0)
                bit_at = pl.multiple_of(s * 2 * half + h * half + t * tile, tile)
                acc_ref[...] += product(positive, own_bits[:, pl.ds(bit_at, tile)])
                return unused

            lax.fori_loop(0, half // tile, step, 0, unroll=True)

    cuts = width // LANES
    for d in range(slabs):
        for c in range(cuts):
            send_ref[d, c * share : (c + 1) * share] = (
                acc_ref[d * share : (d + 1) * share, c * LANES : (c + 1) * LANES] * scale
            )
    pl.semaphore_wait(barrier, slabs - 1)
    exchange(slabs, me, send_ref, recv_ref, send_sems, recv_sems, True)
    exchange(slabs, me, send_ref, recv_ref, send_sems, recv_sems, False)
    summed = jnp.sum(recv_ref[...], axis=0)
    out_ref[...] = jnp.concatenate([summed[c * share : (c + 1) * share] for c in range(cuts)], axis=1)


def local(event_items, event_sessions, sketch_bits):
    slabs = lax.axis_size("stream")
    slab = event_items.shape[0]
    total_events = slab * slabs
    words, band_size = sketch_bits.shape
    owned = band_size // slabs
    rows, width, half = 128, 256, owned // 4
    me = lax.axis_index("stream")
    own_start = me * owned
    first_id = lax.axis_index("item") * band_size + own_start
    blocks = slab // LANES
    length = total_events // LANES

    dma = pltpu.SemaphoreType.DMA
    all_items, all_sessions, head = pl.pallas_call(
        functools.partial(gather_kernel, slabs, rows, blocks),
        out_shape=(
            jax.ShapeDtypeStruct((slabs, blocks, LANES), jnp.int32),
            jax.ShapeDtypeStruct((slabs, blocks, LANES), jnp.int16),
            jax.ShapeDtypeStruct((8, LANES), jnp.float32),
        ),
        in_specs=[VMEM],
        out_specs=(VMEM, VMEM, VMEM),
        scratch_shapes=[
            pltpu.VMEM((blocks, LANES), jnp.int16),
            pltpu.VMEM((4, 8, LANES), jnp.int32),
            pltpu.VMEM((blocks + 16, LANES), jnp.int32),
            pltpu.VMEM((blocks + 16, LANES), jnp.int32),
            pltpu.VMEM((rows + 8, LANES), jnp.float32),
            pltpu.VMEM((8, LANES), jnp.float32),
            pltpu.VMEM((slabs, 8, LANES), jnp.float32),
            pltpu.VMEM((slabs, 8, LANES), jnp.float32),
            dma((slabs,)),
            dma((slabs,)),
            dma((slabs,)),
            dma((slabs,)),
            dma((4,)),
            dma((4,)),
            dma((slabs,)),
            dma((slabs,)),
        ],
        compiler_params=pltpu.CompilerParams(
            collective_id=0, has_side_effects=True, vmem_limit_bytes=VMEM_GRANT
        ),
        name="gather_events",
    )(jnp.stack([event_items, event_sessions]).reshape(2, blocks, LANES))

    band_rows = max(8, 2 * half // LANES)
    counts, margins = pl.pallas_call(
        functools.partial(tile_kernel, rows, length, half),
        out_shape=(
            jax.ShapeDtypeStruct((2, 2 * rows, half), jnp.float32),
            jax.ShapeDtypeStruct((2, band_rows, LANES), jnp.float32),
        ),
        in_specs=[pl.BlockSpec(memory_space=pltpu.SMEM), VMEM, VMEM],
        out_specs=(VMEM, VMEM),
        scratch_shapes=[
            pltpu.VMEM((length, LANES), jnp.int32),
            pltpu.VMEM((length + 32, LANES), jnp.int32),
            pltpu.VMEM((2, length, LANES), jnp.float32),
        ],
        compiler_params=pltpu.CompilerParams(vmem_limit_bytes=VMEM_GRANT),
        name="tile_counts",
    )(first_id.astype(jnp.int32)[None], all_items, all_sessions)

    own_rows = pl.pallas_call(
        functools.partial(sketch_kernel, slabs, rows, half, width, 1.0 / math.sqrt(total_events)),
        out_shape=jax.ShapeDtypeStruct((rows // slabs, width), jnp.float32),
        in_specs=[VMEM] * 3 + [pl.BlockSpec(memory_space=pl.ANY)],
        out_specs=VMEM,
        scratch_shapes=[
            pltpu.VMEM((2, band_rows, LANES), jnp.float32),
            pltpu.VMEM((words, owned), jnp.int32),
            pltpu.VMEM((words, rows), jnp.int32),
            pltpu.VMEM((rows, width), jnp.float32),
            pltpu.VMEM((slabs, 8, LANES), jnp.float32),
            pltpu.VMEM((slabs, 8, LANES), jnp.float32),
            dma((2,)),
            dma((slabs,)),
            dma((slabs,)),
        ],
        compiler_params=pltpu.CompilerParams(
            collective_id=1, has_side_effects=True, vmem_limit_bytes=VMEM_GRANT
        ),
        name="sketch_tile",
    )(counts, margins, head, sketch_bits)
    if lax.axis_size("item") > 1:
        own_rows = lax.psum(own_rows, "item")
    return own_rows


def solution(mesh):
    placed = (P("stream"), P("stream"), P(None, "item"))
    return jax.shard_map(
        local, mesh=mesh, in_specs=placed, out_specs=P("stream", None), check_vma=False
    )
```
